512 devices in a mesh: seq: 32 (over x, y_hi, core), tp: 16 (over z, y_lo).
Axes of the slice: x: 4, y: 8 (y_hi: 4, y_lo: 2; y = y_hi * 2 + y_lo), z: 8, core: 2. Of those that a mesh axis runs over, the one named last changes fastest.
Arguments:
- hidden: bfloat16 [16384, 4096], P('seq', 'tp'), may hold values from -6 to 6
- norm_gain: float32 [4096], P('tp'), may hold values from 0.5 to 1.5
- rank_down: bfloat16 [4096, 1024], P('tp'), may hold values from -0.09375 to 0.09375
- gate_up: bfloat16 [1024, 4096], P(None, 'tp'), may hold values from -0.1875 to 0.1875
- value_up: bfloat16 [1024, 4096], P(None, 'tp'), may hold values from -0.1875 to 0.1875
- state_up: bfloat16 [1024, 1024], P(None, 'tp'), may hold values from -0.1875 to 0.1875
- step_up: bfloat16 [1024, 64], P(None, 'tp'), may hold values from -0.1875 to 0.1875
- conv_value: float32 [4, 4096], P(None, 'tp'), may hold values from -3 to 3
- conv_state: float32 [4, 1024], P(None, 'tp'), may hold values from -3 to 3
- step_bias: float32 [64], P('tp'), may hold values from -6.9 to -2.3
- decay_log: float32 [64], P('tp'), may hold values from -11 to 2.77
- skip_gain: float32 [64], P('tp'), may hold values from 0.5 to 1.5
- gate_gain: float32 [4096], P('tp'), may hold values from 0.5 to 1.5
- out_down: bfloat16 [4096, 1024], P('tp'), may hold values from -0.09375 to 0.09375
- out_up: bfloat16 [1024, 4096], P(None, 'tp'), may hold values from -0.1875 to 0.1875
Outputs:
- block_out: bfloat16 [16384, 4096], P('seq', 'tp')
The draws below stay inside these ranges and needn't reach their ends.
All inputs are finite; a program needn't handle non-finite values.
Results may differ from the reference program's by a relative error of at most 0.012.
Values may be sent and summed in bfloat16 or wider, within the bound.
A program may use at most 64 MiB of HBM per device.

```python
import jax
import jax.numpy as jnp
from jax import lax

D = 4096
HEAD_DIM = 64
NSTATE = 128
CONV = 4
RANK = 1024
HEADS = 64
GROUPS = 4
TOK_DEV = 512
INNER = 4096
SEQ_LEN = 16384


def levels(rng, extent, cuts, low, largest):
    level = 1.0
    for position, blocks in cuts:
        steps = jax.random.uniform(jax.random.fold_in(jax.random.fold_in(rng, 6), position), (blocks,), jnp.float32, low / len(cuts), largest / len(cuts))
        level = level * jnp.repeat(jnp.exp(steps), extent[position] // blocks).reshape((-1,) + (1,) * (len(extent) - 1 - position))
    return level


def noise(own_key, extent, deviation, reach, split=(), kind=jnp.bfloat16):
    values = deviation * jax.random.normal(own_key, extent, jnp.float32)
    if split:
        values = values * levels(own_key, extent, split, -0.22, 0.18)
    return jnp.clip(values, -reach, reach).astype(kind)


def setup_inputs(seed: int = 0) -> dict:
    key_list = jax.random.split(jax.random.key(seed), 16)
    hidden = noise(key_list[0], (SEQ_LEN, D), 1.0, 6.0, ((0, 32), (1, 16)))
    norm_gain = jnp.clip(1.0 + 0.1 * jax.random.normal(key_list[1], (D,), jnp.float32), 0.5, 1.5)
    rank_down = noise(key_list[2], (D, RANK), D ** -0.5, 0.09375, ((0, 16),))
    gate_up = noise(key_list[3], (RANK, INNER), RANK ** -0.5, 0.1875, ((1, 16),))
    value_up = noise(key_list[4], (RANK, INNER), RANK ** -0.5, 0.1875, ((1, 16),))
    state_up = noise(key_list[5], (RANK, 2 * GROUPS * NSTATE), RANK ** -0.5, 0.1875, ((1, 16),))
    step_up = noise(key_list[6], (RANK, HEADS), RANK ** -0.5, 0.1875, ((1, 16),))
    conv_value = noise(key_list[7], (CONV, INNER), CONV ** -0.5, 3.0, ((1, 16),), jnp.float32)
    conv_state = noise(key_list[8], (CONV, 2 * GROUPS * NSTATE), CONV ** -0.5, 3.0, ((1, 16),), jnp.float32)
    step_bias = jnp.clip(-6.9 + 4.6000001430511475 * jax.random.uniform(key_list[9], (HEADS,), jnp.float32) ** levels(key_list[9], (HEADS,), ((0, 16),), -0.2, 0.2), -6.9, -2.3)
    decay_log = jnp.clip(-11.0 + 13.77 * jax.random.uniform(key_list[10], (HEADS,), jnp.float32) ** levels(key_list[10], (HEADS,), ((0, 16),), -0.2, 0.2), -11.0, 2.77)
    skip_gain = jnp.clip(0.5 + 1.0 * jax.random.uniform(key_list[11], (HEADS,), jnp.float32) ** levels(key_list[11], (HEADS,), ((0, 16),), -0.2, 0.2), 0.5, 1.5)
    gate_gain = jnp.clip(1.0 + 0.1 * jax.random.normal(key_list[12], (INNER,), jnp.float32), 0.5, 1.5)
    out_down = noise(key_list[13], (INNER, RANK), INNER ** -0.5, 0.09375, ((0, 16),))
    out_up = noise(key_list[14], (RANK, D), RANK ** -0.5, 0.1875, ((1, 16),))
    return {"hidden": hidden, "norm_gain": norm_gain, "rank_down": rank_down, "gate_up": gate_up, "value_up": value_up, "state_up": state_up, "step_up": step_up, "conv_value": conv_value, "conv_state": conv_state, "step_bias": step_bias, "decay_log": decay_log, "skip_gain": skip_gain, "gate_gain": gate_gain, "out_down": out_down, "out_up": out_up}


epsilon = 1e-05
highest = lax.Precision.HIGHEST

def depthwise(pre_rows, weights):
    padded = jnp.pad(pre_rows.astype(jnp.float32), ((CONV - 1, 0), (0, 0)))
    length = pre_rows.shape[0]
    result = jnp.zeros(pre_rows.shape, jnp.float32)
    for offset in range(CONV):
        result = result + weights[offset] * padded[offset:offset + length]
    return jax.nn.silu(result).astype(jnp.bfloat16)

def reference(hidden, norm_gain, rank_down, gate_up, value_up, state_up, step_up, conv_value, conv_state, step_bias, decay_log, skip_gain, gate_gain, out_down, out_up):
    blocks = SEQ_LEN // TOK_DEV
    hidden_blocks = hidden.reshape(blocks, TOK_DEV, D)

    def in_block(rows):
        wide_rows = rows.astype(jnp.float32)
        factor = lax.rsqrt(lax.optimization_barrier(jnp.mean(wide_rows * wide_rows, axis=1)) + epsilon)
        scaled = (wide_rows * norm_gain).astype(jnp.bfloat16)
        reduced = (jnp.dot(scaled, rank_down, preferred_element_type=jnp.float32) * factor[:, None]).astype(jnp.bfloat16)
        return tuple((jnp.dot(reduced, weight, preferred_element_type=jnp.float32).astype(jnp.bfloat16) for weight in (gate_up, value_up, state_up, step_up)))
    gate_pre, value_pre, state_pre, step_pre = lax.map(in_block, hidden_blocks)
    value_act = depthwise(value_pre.reshape(SEQ_LEN, INNER), conv_value)
    state_act = depthwise(state_pre.reshape(SEQ_LEN, 2 * GROUPS * NSTATE), conv_state)
    repeat_count = HEADS // GROUPS
    causal = jnp.arange(TOK_DEV)[:, None] >= jnp.arange(TOK_DEV)[None, :]

    def ssd_block(state, inputs):
        value_rows, state_rows, step_rows = inputs
        step_size = jax.nn.softplus(step_rows.astype(jnp.float32) + step_bias)
        log_decay = jnp.cumsum(-jnp.exp(decay_log) * step_size, axis=0)
        values = value_rows.astype(jnp.float32).reshape(TOK_DEV, HEADS, HEAD_DIM)
        projections = state_rows.astype(jnp.float32)
        inward = projections[:, :GROUPS * NSTATE].reshape(TOK_DEV, GROUPS, NSTATE)
        outward = projections[:, GROUPS * NSTATE:].reshape(TOK_DEV, GROUPS, NSTATE)
        inward_heads = jnp.repeat(inward, repeat_count, axis=1)
        outward_heads = jnp.repeat(outward, repeat_count, axis=1)
        coupling = jnp.einsum('tgn,sgn->gts', outward, inward, precision=highest)
        coupling = jnp.repeat(coupling, repeat_count, axis=0)
        spread = log_decay.T[:, :, None] - log_decay.T[:, None, :]
        attenuation = jnp.where(causal[None], jnp.exp(jnp.where(causal[None], spread, 0.0)), 0.0)
        mixing = coupling * attenuation * step_size.T[:, None, :]
        within = jnp.einsum('hts,shp->thp', mixing, values, precision=highest)
        carried_in = jnp.exp(log_decay)[:, :, None] * jnp.einsum('thn,hpn->thp', outward_heads, state, precision=highest)
        mixed = within + carried_in + skip_gain[None, :, None] * values
        ending = jnp.exp(log_decay[-1][None, :] - log_decay) * step_size
        new_state = jnp.exp(log_decay[-1])[:, None, None] * state + jnp.einsum('sh,shp,shn->hpn', ending, values, inward_heads, precision=highest)
        return (new_state, mixed.reshape(TOK_DEV, INNER))
    start_state = jnp.zeros((HEADS, HEAD_DIM, NSTATE), jnp.float32)
    scan_inputs = (value_act.reshape(blocks, TOK_DEV, INNER), state_act.reshape(blocks, TOK_DEV, 2 * GROUPS * NSTATE), step_pre)
    final_state, mixed_blocks = lax.scan(ssd_block, start_state, scan_inputs)

    def out_block(inputs):
        mixed, gate_rows, rows = inputs
        gated = mixed * jax.nn.silu(gate_rows.astype(jnp.float32))
        grouped = gated.reshape(TOK_DEV, GROUPS, INNER // GROUPS)
        factor = lax.rsqrt(lax.optimization_barrier(jnp.mean(grouped * grouped, axis=2)) + epsilon)
        normed = ((grouped * factor[:, :, None]).reshape(TOK_DEV, INNER) * gate_gain).astype(jnp.bfloat16)
        projected = jnp.dot(normed, out_down, preferred_element_type=jnp.float32).astype(jnp.bfloat16)
        update = jnp.dot(projected, out_up, preferred_element_type=jnp.float32)
        return (rows.astype(jnp.float32) + update).astype(jnp.bfloat16)
    outputs = lax.map(out_block, (mixed_blocks, gate_pre, hidden_blocks))
    return outputs.reshape(SEQ_LEN, D)
```

```python
import functools

import jax
import jax.numpy as jnp
from jax import lax
from jax.experimental import pallas as pl
from jax.experimental.pallas import tpu as pltpu
from jax.sharding import Mesh
from jax.sharding import PartitionSpec as P

GROUPS = 4
EPS = 1e-05
SEQ = ("x", "yh", "core")
TP = ("z", "yl")
F32 = jnp.float32
BF16 = jnp.bfloat16
MESH = pl.DeviceIdType.MESH

ORDER = (4, -3, 3, -2, 2, -1, 1, 0)


def nt(a, b):
    return lax.dot_general(a, b, (((1,), (1,)), ((), ())), preferred_element_type=F32)


def nn(a, b):
    return jnp.dot(a, b, preferred_element_type=F32)


def silu(x):
    return x * (1.0 / (1.0 + jnp.exp(-x)))


def split2(x):
    high = x.astype(BF16)
    return high, (x - high.astype(F32)).astype(BF16)


class Copies:
    def __init__(self, send, recv):
        self.send, self.recv, self.used, self.all = send, recv, 0, []

    def make(self, src, dst, **where):
        k = self.used
        self.used += 1
        copy = pltpu.make_async_remote_copy(
            src_ref=src,
            dst_ref=dst,
            send_sem=self.send.at[k],
            recv_sem=self.recv.at[k],
            device_id=where,
            device_id_type=MESH,
        )
        self.all.append(copy)
        return copy

    def go(self, src, dst, **where):
        copy = self.make(src, dst, **where)
        copy.start()
        return copy

    def drain(self):
        for copy in self.all:
            copy.wait_send()
        self.all = []


def reduce_scatter(cp, z, y, nz, pa, pb, ya, ra, la, rb, lb, yb, ysend, hooks):
    at = lambda off: lax.rem(z + off + nz, nz)
    right, left, other = at(1), at(-1), 1 - y
    up = lambda v: v.astype(F32)
    across = {}
    for k, off in enumerate(ORDER):
        across[off] = (k, cp.go(pa.at[at(off), other], ya.at[k], yl=other))
    br = cp.go(pb.at[at(4)], rb.at[0], z=right)
    bl = cp.go(pb.at[at(-3)], lb.at[0], z=left)
    hooks[0]()

    def own(off):
        k, copy = across[off]
        copy.wait_recv()
        return up(pa[at(off), y]) + up(ya[k])

    pa[at(4), y] = own(4).astype(BF16)
    ar = cp.go(pa.at[at(4), y], ra.at[0], z=right)
    pa[at(-3), y] = own(-3).astype(BF16)
    al = cp.go(pa.at[at(-3), y], la.at[0], z=left)
    for s in (1, 2, 3):
        br.wait_recv()
        rb[s - 1] = (up(rb[s - 1]) + up(pb[at(4 - s)])).astype(BF16)
        br = cp.go(rb.at[s - 1], rb.at[s], z=right)
        if s < 3:
            bl.wait_recv()
            lb[s - 1] = (up(lb[s - 1]) + up(pb[at(s - 3)])).astype(BF16)
            bl = cp.go(lb.at[s - 1], lb.at[s], z=left)
        mine = own(4 - s)
        ar.wait_recv()
        ra[s - 1] = (up(ra[s - 1]) + mine).astype(BF16)
        ar = cp.go(ra.at[s - 1], ra.at[s], z=right)
        if s < 3:
            mine = own(s - 3)
            al.wait_recv()
            la[s - 1] = (up(la[s - 1]) + mine).astype(BF16)
            al = cp.go(la.at[s - 1], la.at[s], z=left)
        hooks[s]()
    br.wait_recv()
    bl.wait_recv()
    ysend[...] = (up(pb[z, other]) + up(rb[3, other]) + up(lb[2, other])).astype(BF16)
    by = cp.go(ysend, yb, yl=other)
    mine = own(0)
    ar.wait_recv()
    al.wait_recv()
    total_a = mine + up(ra[3]) + up(la[2])
    total_b = up(pb[z, y]) + up(rb[3, y]) + up(lb[2, y])
    by.wait_recv()
    return total_a, total_b + up(yb[...])


def all_gather(cp, z, y, nz, ga, gb):
    at = lambda off: lax.rem(z + off + nz, nz)
    right, left, other = at(1), at(-1), 1 - y
    by = cp.go(gb.at[z, y], gb.at[z, y], yl=other)
    ar = cp.go(ga.at[z, y], ga.at[z, y], z=right)
    al = cp.go(ga.at[z, y], ga.at[z, y], z=left)
    across = [cp.go(ga.at[z, y], ga.at[z, y], yl=other)]
    by.wait_recv()
    br = cp.go(gb.at[z], gb.at[z], z=right)
    bl = cp.go(gb.at[z], gb.at[z], z=left)
    for s in (1, 2, 3, 4):
        ar.wait_recv()
        block = ga.at[at(-s), y]
        if s < 4:
            ar = cp.go(block, block, z=right)
        across.append(cp.go(block, block, yl=other))
        if s < 4:
            al.wait_recv()
            block = ga.at[at(s), y]
            if s < 3:
                al = cp.go(block, block, z=left)
            across.append(cp.go(block, block, yl=other))
        br.wait_recv()
        if s < 4:
            br = cp.go(gb.at[at(-s)], gb.at[at(-s)], z=right)
            bl.wait_recv()
            if s < 3:
                bl = cp.go(gb.at[at(s)], gb.at[at(s)], z=left)
    for copy in across:
        copy.wait_recv()


def gather_scan(cp, buf, place, peers, axis):
    copies = []
    for o in range(1, peers):
        there = lax.rem(place + o, peers)
        copies.append(cp.go(buf.at[place], buf.at[place], **{axis: there}))
    return copies


def pack(ref, where, state, decay):
    high, low = split2(decay)
    ref[where, pl.ds(0, 128), :] = state.astype(BF16)
    row = lax.broadcasted_iota(jnp.int32, (16, 128), 0)
    tail = jnp.where(row == 0, high.astype(F32), jnp.where(row == 1, low.astype(F32), 0.0))
    ref[where, pl.ds(128, 16), :] = tail.astype(BF16)


def unpack(ref, where):
    tail = ref[where, pl.ds(128, 16), :].astype(F32)
    return ref[where, pl.ds(0, 128), :].astype(F32), tail[0:1] + tail[1:2]


def prefix(buf, place, peers):
    run, decay = jnp.zeros((128, 128), F32), jnp.ones((1, 128), F32)
    before, before_decay = run, decay
    for k in range(peers):
        here = place == k
        before = jnp.where(here, run, before)
        before_decay = jnp.where(here, decay, before_decay)
        state, d = unpack(buf, k)
        run, decay = d * run + state, d * decay
    return before, before_decay, run, decay


def seq_shift(sizes, place, by):
    nx, nyh, ncore = sizes[:3]
    total = nx * nyh * ncore
    there = lax.rem(place + by + total, total)
    return dict(x=there // (nyh * ncore), yh=lax.rem(there // ncore, nyh), core=lax.rem(there, ncore))


def token_rows(v):
    return jnp.concatenate([v[0:1, 128 * c : 128 * c + 128] for c in range(v.shape[1] // 128)], axis=0)


def halves(low, high):
    lane = lax.broadcasted_iota(jnp.int32, (low.shape[0], 128), 1)
    return jnp.where(lane < 64, low, high)


def block_kernel(sizes, names, *args):
    r = dict(zip(names, args))
    nx, nyh, ncore, nz, nyl = sizes
    x, yh, core, z, y = (lax.axis_index(a) for a in ("x", "yh", "core", "z", "yl"))
    other, twin = 1 - y, 1 - core
    hid, pa, pb, ga, gb = r["hid"], r["pa"], r["pb"], r["ga"], r["gb"]
    tokens, width = hid.shape
    ca, rows, rank = pa.shape[3], pa.shape[2], r["down"].shape[1]
    place = (x * nyh + yh) * ncore + core
    at = lambda off: lax.rem(z + off + nz, nz)
    mate = z + 1 - 2 * lax.rem(z, 2)
    cp = Copies(r["send"], r["recv"])

    shares = [(o, c) for o in range(nx) for c in range(ncore) if o or c]
    share_peer = lambda o, c: dict(x=lax.rem(x + o, nx), core=lax.rem(core + c, ncore))
    peers = [dict(z=at(o)) for o in range(1, nz)] + [dict(yl=other), dict(z=mate, yl=other)]
    peers += [dict(yh=lax.rem(yh + o, nyh)) for o in range(1, nyh)]
    peers += [share_peer(o, c) for o, c in shares]
    peers += [seq_shift(sizes, place, 1), seq_shift(sizes, place, -1)]
    barrier = pltpu.get_barrier_semaphore()
    for peer in peers:
        pl.semaphore_signal(barrier, inc=1, device_id=peer, device_id_type=MESH)

    loads = {}
    for k, name in enumerate(("hid", "down", "state_w", "value_w", "step_w", "gate_w", "odown", "oup")):
        loads[name] = pltpu.make_async_copy(r[name + "_h"], r[name], r["load_sem"].at[k])
        loads[name].start()

    loads["hid"].wait()
    loads["down"].wait()
    wide = hid[...].astype(F32)
    ones = jnp.ones((8, width), BF16)
    high, low = split2(wide * wide)
    squares = token_rows(nt(ones, high) + nt(ones, low))
    taps = r["conv_s"][...]
    blank = jnp.zeros_like(taps)
    taps = jnp.where(y == 0, jnp.concatenate([taps, blank], axis=1), jnp.concatenate([blank, taps], axis=1))
    r["q0"][...] = jnp.concatenate([squares, taps], axis=0)
    part = nn((wide * r["gain"][...]).astype(BF16), r["down"][...]).astype(BF16)
    pa[...] = part[:, :ca].reshape(pa.shape)
    pb[...] = part[:, ca:].reshape(pb.shape)
    share = x * ncore + core
    half = r["state_w"].shape[1]
    span = rank // (nx * ncore)
    eye = (lax.broadcasted_iota(jnp.int32, (half, half), 0) == lax.broadcasted_iota(jnp.int32, (half, half), 1)).astype(BF16)
    loads["state_w"].wait()
    gz = r["gz"]
    gz[z] = nt(eye, r["state_w"][pl.ds(pl.multiple_of(share * span, span), span), :]).astype(BF16)
    pl.semaphore_wait(barrier, len(peers))

    picked = z // 2
    held = {}

    def hook0():
        held["q"] = cp.go(r["q0"], r["q1"], yl=other)
        held["gz"] = []
        for o in range(1, nz):
            copy = cp.make(gz.at[z], gz.at[z], z=at(o))
            cp.all.pop()
            sends = at(o) // 2 == lax.rem(z, 4)
            comes = lax.rem(at(-o), 4) == picked
            held["gz"].append((sends, comes, copy))

            @pl.when(sends)
            def _():
                copy.start()

    def hook1():
        held["q"].wait_recv()
        r["qz"][z] = r["q0"][...] + r["q1"][...]
        held["qz"] = [cp.go(r["qz"].at[z], r["qz"].at[z], z=at(o)) for o in range(1, nz)]

    def hook2():
        for sends, comes, copy in held["gz"]:
            @pl.when(comes)
            def _():
                copy.wait_recv()

            @pl.when(sends)
            def _():
                copy.wait_send()

        for k in range(2):
            r["ss"][share, k, y] = gz[4 * k + picked]
        held["ss"] = cp.go(r["ss"].at[share, :, y], r["ss"].at[share, :, y], yl=other)

    def hook3():
        held["ss"].wait_recv()
        held["shares"] = [cp.go(r["ss"].at[share], r["ss"].at[share], **share_peer(o, c)) for o, c in shares]

    total_a, total_b = reduce_scatter(
        cp, z, y, nz, pa, pb, *(r[n] for n in ("ya", "ra", "la", "rb", "lb", "yb", "ysend")), (hook0, hook1, hook2, hook3)
    )
    for copy in held["qz"]:
        copy.wait_recv()
    block = 2 * z + y
    summed = r["qz"][0]
    for k in range(1, nz):
        summed = summed + r["qz"][k]
    row = jnp.zeros((1, 128), F32)
    per = 128 // rows
    for c in range(tokens // 128):
        row = jnp.where(block // per == c, summed[c : c + 1], row)
    wanted = lax.broadcasted_iota(jnp.int32, (rows, 128), 1) == lax.broadcasted_iota(jnp.int32, (rows, 128), 0) + rows * lax.rem(block, per)
    mean = jnp.sum(jnp.where(wanted, row, 0.0), axis=1, keepdims=True) / (width * nz * nyl)
    factor = lax.rsqrt(mean + EPS)
    ga[z, y] = (total_a * factor).astype(BF16)
    gb[z, y] = (total_b * factor).astype(BF16)
    all_gather(cp, z, y, nz, ga, gb)

    last = pl.ds(rows - 16, 16)
    following = seq_shift(sizes, place, 1)
    ha = cp.go(ga.at[nz - 1, 1, last], r["halo_a"], **following)
    hb = cp.go(gb.at[nz - 1, 1, last], r["halo_b"], **following)
    red_a, red_b = ga[...].reshape(tokens, ca), gb[...].reshape(tokens, rank - ca)

    for copy in held["shares"]:
        copy.wait_recv()
    swt = r["swt"]
    for k in range(nx * ncore):
        swt[:, span * k : span * (k + 1)] = r["ss"][k].reshape(2 * nyl * half, span)
    pre = r["pre"]
    chans = 2 * nyl * half
    for name in ("value_w", "step_w", "gate_w"):
        loads[name].wait()
    value_w = r["value_w"]

    def project(a, b):
        values = nn(a, value_w[:ca]) + nn(b, value_w[ca:])
        states = nt(a, swt[:, :ca]) + nt(b, swt[:, ca:])
        return values, states

    pre[16:, :width], pre[16:, width:] = project(red_a, red_b)

    heads = r["step_w"].shape[1]
    put = (lax.broadcasted_iota(jnp.int32, (8, heads), 0) == lax.broadcasted_iota(jnp.int32, (8, heads), 1)).astype(BF16)
    step_t = nt(put, r["step_w"][...]).astype(BF16)
    raw = nt(step_t[:, :ca], red_a) + nt(step_t[:, ca:], red_b)
    head = lax.broadcasted_iota(jnp.int32, (8, 1), 0)
    bias, decay = jnp.zeros((8, 1), F32), jnp.zeros((8, 1), F32)
    for h in range(heads):
        bias = jnp.where(head == h, r["bias"][h], bias)
        decay = jnp.where(head == h, r["decay"][h], decay)
    raw = raw + bias
    step = jnp.maximum(raw, 0.0) + jnp.log1p(jnp.exp(-jnp.abs(raw)))
    lane = lax.broadcasted_iota(jnp.int32, (8, tokens), 1)
    logs = -jnp.exp(decay) * step
    k = 1
    while k < tokens:
        logs = logs + jnp.where(lane >= k, pltpu.roll(logs, k, axis=1), 0.0)
        k *= 2
    final = logs[:, tokens - 1 : tokens]
    ending = jnp.exp(final - logs) * step
    stack = jnp.concatenate([logs, ending, jnp.exp(logs), jnp.zeros((104, tokens), F32)], axis=0)
    cols = r["cols"]
    cols[...] = stack.T
    whole = jnp.exp(final)

    ha.wait_recv()
    hb.wait_recv()
    hv, hs = project(r["halo_a"][...], r["halo_b"][...])
    keep = jnp.where(place == 0, 0.0, 1.0)
    pre[:16, :width] = hv * keep
    pre[:16, width:] = hs * keep
    vact, bact, cact = r["vact"], r["bact"], r["cact"]
    weights = r["conv_v"][...]
    sweights = jnp.concatenate([r["qz"][picked][4:8], r["qz"][4 + picked][4:8]], axis=1)
    for c in range(tokens // 128):
        acc_v = jnp.zeros((128, width), F32)
        acc_s = jnp.zeros((128, chans), F32)
        for t in range(4):
            window = pre[13 + t + 128 * c : 13 + t + 128 * c + 128, :]
            acc_v = acc_v + weights[t : t + 1] * window[:, :width]
            acc_s = acc_s + sweights[t : t + 1] * window[:, width:]
        here = slice(128 * c, 128 * c + 128)
        vact[here] = silu(acc_v).astype(BF16)
        acts = silu(acc_s).astype(BF16)
        bact[here] = acts[:, :128]
        cact[here] = acts[:, 128:]

    eye = (lax.broadcasted_iota(jnp.int32, (128, 128), 0) == lax.broadcasted_iota(jnp.int32, (128, 128), 1)).astype(BF16)
    b_t = nt(eye, bact[...]).astype(BF16)
    own_state, own_decay = [], []
    for p in range(2):
        h = 2 * p
        ends = halves(cols[:, 8 + h : 9 + h], cols[:, 9 + h : 10 + h])
        scaled = (vact[:, 128 * p : 128 * p + 128].astype(F32) * ends).astype(BF16)
        own_state.append(nn(b_t, scaled))
        own_decay.append(halves(whole[h : h + 1], whole[h + 1 : h + 2]))
    theirs = lambda a, b, c: jnp.where(c == 0, a, b)
    one_send, one_recv = r["one"].at[0], r["one"].at[1]
    pack(r["one"], 0, theirs(*own_state, twin), theirs(*own_decay, twin))
    first = cp.go(one_send, one_recv, core=twin)
    mine, mine_decay = theirs(*own_state, core), theirs(*own_decay, core)
    gates = nn(red_a, r["gate_w"][:ca]) + nn(red_b, r["gate_w"][ca:])
    r["gact"][...] = silu(gates)
    first.wait_recv()
    got, got_decay = unpack(r["one"], 1)
    state0, state1 = jnp.where(core == 0, mine, got), jnp.where(core == 0, got, mine)
    decay0, decay1 = jnp.where(core == 0, mine_decay, got_decay), jnp.where(core == 0, got_decay, mine_decay)
    pack(r["two"], yh, decay1 * state0 + state1, decay0 * decay1)
    second = gather_scan(cp, r["two"], yh, nyh, "yh")

    mix = r["mix"]
    for c in range(tokens // 128):
        here = slice(128 * c, 128 * c + 128)
        past = 128 * c + 128
        couple = nt(cact[here], bact[:past])
        seen = lax.broadcasted_iota(jnp.int32, (128, past), 0) + 128 * c >= lax.broadcasted_iota(jnp.int32, (128, past), 1)
        for p in range(2):
            outs = []
            for h in (2 * p, 2 * p + 1):
                spread = cols[here, h : h + 1] - logs[h : h + 1, :past]
                fade = jnp.where(seen, jnp.exp(jnp.minimum(spread, 0.0)), 0.0)
                m = (couple * fade * step[h : h + 1, :past]).astype(BF16)
                outs.append(nn(m, vact[:past, 128 * p : 128 * p + 128]))
            skip = halves(jnp.full((1, 1), r["skip"][2 * p], F32), jnp.full((1, 1), r["skip"][2 * p + 1], F32))
            values = vact[here, 128 * p : 128 * p + 128].astype(F32)
            mix[here, 128 * p : 128 * p + 128] = halves(*outs) + skip * values

    for copy in second:
        copy.wait_recv()
    before, before_decay, run, run_decay = prefix(r["two"], yh, nyh)
    pack(r["three"], x, run, run_decay)
    third = gather_scan(cp, r["three"], x, nx, "x")
    for copy in third:
        copy.wait_recv()
    far = prefix(r["three"], x, nx)[0]
    entry0 = before_decay * far + before
    entry1 = decay0 * entry0 + state0
    inc = r["inc"]
    inc[core] = theirs(entry0, entry1, core).astype(BF16)
    r["fin"][...] = theirs(entry0, entry1, twin).astype(BF16)
    fourth = cp.go(r["fin"], inc.at[core], core=twin)
    fourth.wait_recv()

    gated = []
    for p in range(2):
        h = 2 * p
        carried = nn(cact[...], inc[p]) * halves(cols[:, 16 + h : 17 + h], cols[:, 17 + h : 18 + h])
        gated.append((mix[:, 128 * p : 128 * p + 128] + carried) * r["gact"][:, 128 * p : 128 * p + 128])
    gated = jnp.concatenate(gated, axis=1)
    high, low = split2(gated * gated)
    own = token_rows(nt(ones, high) + nt(ones, low))
    r["gq"][0] = jnp.concatenate([own, jnp.zeros_like(own)], axis=0)
    groups = [
        cp.go(r["gq"].at[0], r["gq"].at[1], yl=other),
        cp.go(r["gq"].at[0], r["gq"].at[2], z=mate),
        cp.go(r["gq"].at[0], r["gq"].at[3], z=mate, yl=other),
    ]
    loads["odown"].wait()
    pf = r["pf"]
    pf[...] = nn((gated * r["gain2"][...]).astype(BF16), r["odown"][...])
    for copy in groups:
        copy.wait_recv()
    squares = r["gq"][0] + r["gq"][1] + r["gq"][2] + r["gq"][3]
    norm = lax.rsqrt(squares / (width * 4) + EPS)
    norm = jnp.concatenate([norm, jnp.zeros((120, 128), F32)], axis=0).T
    per = 128 // (2 * rows)
    pa2, pb2 = r["pa2"], r["pb2"]
    for c in range(tokens // 128):
        scaled = (pf[128 * c : 128 * c + 128, :] * norm[:, c : c + 1]).astype(BF16)
        pa2[per * c : per * c + per] = scaled[:, :ca].reshape(per, *pa2.shape[1:])
        pb2[per * c : per * c + per] = scaled[:, ca:].reshape(per, *pb2.shape[1:])
    nothing = lambda: None
    total_a, total_b = reduce_scatter(
        cp, z, y, nz, pa2, pb2, *(r[n] for n in ("ya2", "ra2", "la2", "rb2", "lb2", "yb2", "ysend2")), (nothing,) * 4
    )
    ga2, gb2 = r["ga2"], r["gb2"]
    ga2[z, y] = total_a.astype(BF16)
    gb2[z, y] = total_b.astype(BF16)
    all_gather(cp, z, y, nz, ga2, gb2)
    loads["oup"].wait()
    oup = r["oup"]
    update = nn(ga2[...].reshape(tokens, ca), oup[:ca]) + nn(gb2[...].reshape(tokens, rank - ca), oup[ca:])
    r["out"][...] = (hid[...].astype(F32) + update).astype(BF16)
    cp.drain()


def on_device(sizes, hidden, norm_gain, rank_down, gate_up, value_up, state_up, step_up, conv_value, conv_state, step_bias, decay_log, skip_gain, gate_gain, out_down, out_up):
    nx, nyh, ncore, nz, nyl = sizes
    tokens, width = hidden.shape
    rank = rank_down.shape[1]
    half = state_up.shape[1]
    rows = tokens // (nz * nyl)
    ca = rank * 5 // 8
    cb = rank - ca
    vm, hbm, sm = (pl.BlockSpec(memory_space=s) for s in (pltpu.VMEM, pl.ANY, pltpu.SMEM))
    operands = [
        ("hid_h", hbm, hidden), ("gain", vm, norm_gain.reshape(1, -1)), ("down_h", hbm, rank_down), ("gate_w_h", hbm, gate_up),
        ("value_w_h", hbm, value_up), ("state_w_h", hbm, state_up), ("step_w_h", hbm, step_up), ("conv_v", vm, conv_value),
        ("conv_s", vm, conv_state), ("bias", sm, step_bias), ("decay", sm, decay_log), ("skip", sm, skip_gain),
        ("gain2", vm, gate_gain.reshape(1, -1)), ("odown_h", hbm, out_down), ("oup_h", hbm, out_up),
    ]
    like = lambda a: pltpu.VMEM(a.shape, a.dtype)
    half_sums = lambda t: [
        ("pa" + t, pltpu.VMEM((nz, 2, rows, ca), BF16)), ("pb" + t, pltpu.VMEM((nz, 2, rows, cb), BF16)),
        ("ya" + t, pltpu.VMEM((nz, rows, ca), BF16)), ("ra" + t, pltpu.VMEM((4, rows, ca), BF16)), ("la" + t, pltpu.VMEM((3, rows, ca), BF16)),
        ("rb" + t, pltpu.VMEM((4, 2, rows, cb), BF16)), ("lb" + t, pltpu.VMEM((3, 2, rows, cb), BF16)),
        ("yb" + t, pltpu.VMEM((rows, cb), BF16)), ("ysend" + t, pltpu.VMEM((rows, cb), BF16)),
        ("ga" + t, pltpu.VMEM((nz, 2, rows, ca), BF16)), ("gb" + t, pltpu.VMEM((nz, 2, rows, cb), BF16)),
    ]
    count = 160
    scratch = [
        ("hid", like(hidden)), ("down", like(rank_down)), ("gate_w", like(gate_up)), ("value_w", like(value_up)), ("state_w", like(state_up)),
        ("step_w", like(step_up)), ("odown", like(out_down)), ("oup", like(out_up)), *half_sums(""), *half_sums("2"),
        ("q0", pltpu.VMEM((8, 128), F32)), ("q1", pltpu.VMEM((8, 128), F32)), ("qz", pltpu.VMEM((nz, 8, 128), F32)),
        ("gz", pltpu.VMEM((nz, half, rank // (nx * ncore)), BF16)), ("ss", pltpu.VMEM((nx * ncore, 2, nyl, half, rank // (nx * ncore)), BF16)),
        ("swt", pltpu.VMEM((2 * nyl * half, rank), BF16)), ("halo_a", pltpu.VMEM((16, ca), BF16)), ("halo_b", pltpu.VMEM((16, cb), BF16)),
        ("pre", pltpu.VMEM((16 + tokens, width + 2 * nyl * half), F32)), ("vact", pltpu.VMEM((tokens, width), BF16)),
        ("bact", pltpu.VMEM((tokens, 128), BF16)), ("cact", pltpu.VMEM((tokens, 128), BF16)), ("gact", pltpu.VMEM((tokens, width), F32)),
        ("cols", pltpu.VMEM((tokens, 128), F32)), ("mix", pltpu.VMEM((tokens, width), F32)), ("pf", pltpu.VMEM((tokens, rank), F32)),
        ("one", pltpu.VMEM((2, 144, 128), BF16)), ("two", pltpu.VMEM((nyh, 144, 128), BF16)), ("three", pltpu.VMEM((nx, 144, 128), BF16)),
        ("fin", pltpu.VMEM((128, 128), BF16)), ("inc", pltpu.VMEM((2, 128, 128), BF16)), ("gq", pltpu.VMEM((4, 8, 128), F32)),
        ("send", pltpu.SemaphoreType.DMA((count,))), ("recv", pltpu.SemaphoreType.DMA((count,))), ("load_sem", pltpu.SemaphoreType.DMA((8,))),
    ]
    names = [n for n, _, _ in operands] + ["out"] + [n for n, _ in scratch]
    return pl.pallas_call(
        functools.partial(block_kernel, sizes, names),
        out_shape=jax.ShapeDtypeStruct(hidden.shape, BF16),
        in_specs=[s for _, s, _ in operands],
        out_specs=vm,
        scratch_shapes=[s for _, s in scratch],
        compiler_params=pltpu.CompilerParams(collective_id=0, has_side_effects=True, vmem_limit_bytes=60 * 2**20),
    )(*(a for _, _, a in operands))


def grid_sizes(mesh):
    seq, tp = mesh.shape["seq"], mesh.shape["tp"]
    nx = nyh = 1
    if seq == 32:
        nx = nyh = 4
    return (nx, nyh, 2, tp // 2, 2)


def solution(mesh):
    sizes = grid_sizes(mesh)
    finer = Mesh(mesh.devices.reshape(sizes), SEQ + TP)
    rows, cols, flat = P(TP, None), P(None, TP), P(TP)
    placed = (P(SEQ, TP), flat, rows, cols, cols, cols, cols, cols, cols, flat, flat, flat, flat, rows, cols)
    return jax.shard_map(
        functools.partial(on_device, sizes), mesh=finer, in_specs=placed, out_specs=P(SEQ, TP), check_vma=False
    )
```

```python
import functools

import jax
import jax.numpy as jnp
from jax import lax
from jax.experimental import pallas as pl
from jax.experimental.pallas import tpu as pltpu
from jax.sharding import Mesh
from jax.sharding import PartitionSpec as P

GROUPS = 4
EPS = 1e-05
SEQ = ("x", "yh", "core")
TP = ("z", "yl")
F32 = jnp.float32
BF16 = jnp.bfloat16
MESH = pl.DeviceIdType.MESH

ORDER = (3, -3, 4, 2, -2, 1, -1, 0)
SKIP = (True, True)
PARTS = (("y", 256), ("y", 256), ("y", 256), ("z", 256))


def nt(a, b):
    return lax.dot_general(a, b, (((1,), (1,)), ((), ())), preferred_element_type=F32)


def nn(a, b):
    return jnp.dot(a, b, preferred_element_type=F32)


def silu(x):
    return x * (1.0 / (1.0 + jnp.exp(-x)))


def split2(x):
    high = x.astype(BF16)
    return high, (x - high.astype(F32)).astype(BF16)


class Copies:
    def __init__(self, send, recv):
        self.send, self.recv, self.used, self.all = send, recv, 0, []

    def make(self, src, dst, **where):
        k = self.used
        self.used += 1
        copy = pltpu.make_async_remote_copy(
            src_ref=src,
            dst_ref=dst,
            send_sem=self.send.at[k],
            recv_sem=self.recv.at[k],
            device_id=where,
            device_id_type=MESH,
        )
        self.all.append(copy)
        return copy

    def go(self, src, dst, **where):
        copy = self.make(src, dst, **where)
        copy.start()
        return copy

    def drain(self):
        for copy in self.all:
            copy.wait_send()
        self.all = []


def up(v):
    return v.astype(F32)


def flow_y_first(cp, env, buf, scale, factor, done):
    z, y, nz = env
    at = lambda off: lax.rem(z + off + nz, nz)
    other = 1 - y
    p, yr, r, h, g = buf["p"], buf["y"], buf["r"], buf["h"], buf["g"]
    part = {1: pl.ds(0, 16), -1: pl.ds(16, 16)}
    across, got = {}, {}
    for k, off in enumerate(ORDER):
        across[off] = (k, cp.go(p.at[at(off), other], yr.at[k], yl=other))
        if k == 2:
            yield
    yield

    def own(off):
        k, copy = across[off]
        copy.wait_recv()
        sums = up(p[at(off), y]) + up(yr[k])
        return sums if scale is None else sums * scale[at(off), y][:, :1]

    for d, s in ((0, 1), (1, -1)):
        p[at(3 * s), y] = own(3 * s).astype(BF16)
        got[s, 3] = cp.go(p.at[at(3 * s), y], r.at[d, 0], z=at(s))
    p[at(4), y] = own(4).astype(BF16)
    for s in (1, -1):
        got[s, 4] = cp.go(p.at[at(4), y, part[s]], h.at[part[s]], z=at(2 * s))
    yield
    far = 2 if SKIP[0] else 1
    for d, s in ((0, 1), (1, -1)):
        mine = own(2 * s)
        got[s, 3].wait_recv()
        got[s, 4].wait_recv()
        r[d, 0] = (up(r[d, 0]) + mine).astype(BF16)
        r[d, 0, part[s]] = (up(r[d, 0, part[s]]) + up(h[part[s]])).astype(BF16)
        got[s, 2] = cp.go(r.at[d, 0], r.at[d, 1], z=at(far * s))
        if SKIP[0]:
            p[at(s), y] = own(s).astype(BF16)
            got[s, 1] = cp.go(p.at[at(s), y], r.at[d, 2], z=at(s))
    yield
    if not SKIP[0]:
        for d, s in ((0, 1), (1, -1)):
            mine = own(s)
            got[s, 2].wait_recv()
            r[d, 1] = (up(r[d, 1]) + mine).astype(BF16)
            got[s, 1] = cp.go(r.at[d, 1], r.at[d, 2], z=at(s))
        yield
    total = own(0)
    for d, s in ((0, 1), (1, -1)):
        for e in (1, 2) if SKIP[0] else (2,):
            got[s, 3 - e].wait_recv()
            total = total + up(r[d, e])
    if factor is not None:
        total = total * factor()[y]
    mine = g.at[z, y]
    g[z, y] = total.astype(BF16)
    seen = {}
    for hop in (1, 2) if SKIP[1] else (1,):
        for s in (1, -1):
            seen[s, hop] = cp.go(mine, mine, z=at(hop * s))
    last = [cp.go(mine, mine, yl=other)]
    yield
    for k in (1, 2, 3):
        for s in (1, -1):
            seen[s, k].wait_recv()
            block = g.at[at(-k * s), y]
            if k == 1 and not SKIP[1]:
                seen[s, 2] = cp.go(block, block, z=at(s))
            if k == 2:
                half = g.at[at(-2 * s), y, part[s]]
                seen[s, 4] = cp.go(half, half, z=at(2 * s))
                seen[s, 3] = cp.go(block, block, z=at(s))
            last.append(cp.go(block, block, yl=other))
        yield
    for s in (1, -1):
        seen[s, 4].wait_recv()
        half = g.at[at(4), y, part[s]]
        last.append(cp.go(half, half, yl=other))
    yield
    for copy in last:
        copy.wait_recv()
    done()


def flow_z_first(cp, env, buf, scale, factor, done):
    z, y, nz = env
    at = lambda off: lax.rem(z + off + nz, nz)
    p, yr, r, h, g = buf["p"], buf["y"], buf["r"], buf["h"], buf["g"]
    part = {1: pl.ds(0, 16), -1: pl.ds(16, 16)}
    every = slice(None)
    got, seen = {}, {}
    for d, s in ((0, 1), (1, -1)):
        got[s, 3] = cp.go(p.at[at(3 * s)], r.at[d, 0], z=at(s))
        got[s, 4] = cp.go(p.at[at(4), :, part[s]], h.at[:, part[s]], z=at(2 * s))
    yield
    far = 2 if SKIP[0] else 1
    for d, s in ((0, 1), (1, -1)):
        got[s, 3].wait_recv()
        got[s, 4].wait_recv()
        r[d, 0] = (up(r[d, 0]) + up(p[at(2 * s)])).astype(BF16)
        r[d, 0, :, part[s]] = (up(r[d, 0, :, part[s]]) + up(h[:, part[s]])).astype(BF16)
        got[s, 2] = cp.go(r.at[d, 0], r.at[d, 1], z=at(far * s))
        if SKIP[0]:
            got[s, 1] = cp.go(p.at[at(s)], r.at[d, 2], z=at(s))
    yield
    if not SKIP[0]:
        for d, s in ((0, 1), (1, -1)):
            got[s, 2].wait_recv()
            r[d, 1] = (up(r[d, 1]) + up(p[at(s)])).astype(BF16)
            got[s, 1] = cp.go(r.at[d, 1], r.at[d, 2], z=at(s))
        yield
    total = up(p[z])
    for d, s in ((0, 1), (1, -1)):
        for e in (1, 2) if SKIP[0] else (2,):
            got[s, 3 - e].wait_recv()
            total = total + up(r[d, e])
    yr[0] = total.astype(BF16)
    swap = cp.go(yr.at[0], yr.at[1], yl=1 - y)
    yield
    swap.wait_recv()
    total = up(yr[0]) + up(yr[1])
    if factor is not None:
        total = total * factor()[...]
    g[z] = total.astype(BF16)
    for hop in (1, 2) if SKIP[1] else (1,):
        for s in (1, -1):
            seen[s, hop] = cp.go(g.at[z], g.at[z], z=at(hop * s))
    yield
    for k in (1, 2, 3):
        for s in (1, -1):
            seen[s, k].wait_recv()
            block = g.at[at(-k * s)]
            if k == 1 and not SKIP[1]:
                seen[s, 2] = cp.go(block, block, z=at(s))
            if k == 2:
                half = g.at[at(-2 * s), :, part[s]]
                seen[s, 4] = cp.go(half, half, z=at(2 * s))
                seen[s, 3] = cp.go(block, block, z=at(s))
        yield
    for s in (1, -1):
        seen[s, 4].wait_recv()
    done()


def run_flows(flows, hooks):
    turn = 0
    while flows:
        left = []
        for flow in flows:
            if next(flow, flow) is not flow:
                left.append(flow)
        flows = left
        if turn < len(hooks):
            hooks[turn]()
        turn += 1


def gather_scan(cp, buf, place, peers, axis):
    copies = []
    for o in sorted(range(1, peers), key=lambda o: -min(o, peers - o)):
        there = lax.rem(place + o, peers)
        copies.append(cp.go(buf.at[place], buf.at[place], **{axis: there}))
    return copies


def pack(ref, where, state, decay):
    high, low = split2(decay)
    ref[where, pl.ds(0, 128), :] = state.astype(BF16)
    row = lax.broadcasted_iota(jnp.int32, (16, 128), 0)
    tail = jnp.where(row == 0, high.astype(F32), jnp.where(row == 1, low.astype(F32), 0.0))
    ref[where, pl.ds(128, 16), :] = tail.astype(BF16)


def unpack(ref, where):
    tail = ref[where, pl.ds(128, 16), :].astype(F32)
    return ref[where, pl.ds(0, 128), :].astype(F32), tail[0:1] + tail[1:2]


def prefix(buf, place, peers):
    run, decay = jnp.zeros((128, 128), F32), jnp.ones((1, 128), F32)
    before, before_decay = run, decay
    for k in range(peers):
        here = place == k
        before = jnp.where(here, run, before)
        before_decay = jnp.where(here, decay, before_decay)
        state, d = unpack(buf, k)
        run, decay = d * run + state, d * decay
    return before, before_decay, run, decay


FLOWS = {"y": flow_y_first, "z": flow_z_first}


class Column:
    def __init__(self, ref):
        self.ref = ref

    def __getitem__(self, k):
        return self.ref[k][..., :1]


def group_buffers(side, nz, rows):
    out = []
    for i, (order, c) in enumerate(PARTS):
        both = (2, rows, c) if order == "z" else (rows, c)
        shapes = dict(p=(nz, 2, rows, c), g=(nz, 2, rows, c), r=(2, 3, *both), h=both, y=(2, *both) if order == "z" else (nz, *both))
        if side == "in":
            shapes["halo"] = (16, c)
        out += [(f"{side}{i}{k}", pltpu.VMEM(v, BF16)) for k, v in shapes.items()]
    return out


def split_groups(r, side):
    out, start = [], 0
    for i, (order, c) in enumerate(PARTS):
        g = {k: r[f"{side}{i}{k}"] for k in ("p", "g", "r", "h", "y", "halo") if f"{side}{i}{k}" in r}
        out.append(dict(g, order=order, cols=slice(start, start + c)))
        start += c
    return out


def seq_shift(sizes, place, by):
    nx, nyh, ncore = sizes[:3]
    total = nx * nyh * ncore
    there = lax.rem(place + by + total, total)
    return dict(x=there // (nyh * ncore), yh=lax.rem(there // ncore, nyh), core=lax.rem(there, ncore))


def token_rows(v):
    return jnp.concatenate([v[0:1, 128 * c : 128 * c + 128] for c in range(v.shape[1] // 128)], axis=0)


def halves(low, high):
    lane = lax.broadcasted_iota(jnp.int32, (low.shape[0], 128), 1)
    return jnp.where(lane < 64, low, high)


def block_kernel(sizes, names, *args):
    r = dict(zip(names, args))
    nx, nyh, ncore, nz, nyl = sizes
    x, yh, core, z, y = (lax.axis_index(a) for a in ("x", "yh", "core", "z", "yl"))
    other, twin = 1 - y, 1 - core
    hid, groups_in, groups_out = r["hid"], split_groups(r, "in"), split_groups(r, "out")
    tokens, width = hid.shape
    rows, rank = groups_in[0]["p"].shape[2], r["down"].shape[1]
    env = (z, y, nz)
    place = (x * nyh + yh) * ncore + core
    at = lambda off: lax.rem(z + off + nz, nz)
    mate = z + 1 - 2 * lax.rem(z, 2)
    cp = Copies(r["send"], r["recv"])

    shares = [(o, c) for o in range(nx) for c in range(ncore) if o or c]
    share_peer = lambda o, c: dict(x=lax.rem(x + o, nx), core=lax.rem(core + c, ncore))
    peers = [dict(z=at(o)) for o in range(1, nz)] + [dict(yl=other), dict(z=mate, yl=other)]
    peers += [dict(yh=lax.rem(yh + o, nyh)) for o in range(1, nyh)]
    peers += [share_peer(o, c) for o, c in shares]
    peers += [seq_shift(sizes, place, 1), seq_shift(sizes, place, -1)]
    barrier = pltpu.get_barrier_semaphore()
    for peer in peers:
        pl.semaphore_signal(barrier, inc=1, device_id=peer, device_id_type=MESH)

    loads = {}
    for k, name in enumerate(("hid", "down", "state_w", "value_w", "step_w", "gate_w", "odown", "oup")):
        loads[name] = pltpu.make_async_copy(r[name + "_h"], r[name], r["load_sem"].at[k])
        loads[name].start()

    loads["hid"].wait()
    loads["down"].wait()
    wide = hid[...].astype(F32)
    ones = jnp.ones((8, width), BF16)
    high, low = split2(wide * wide)
    squares = token_rows(nt(ones, high) + nt(ones, low))
    taps = r["conv_s"][...]
    blank = jnp.zeros_like(taps)
    taps = jnp.where(y == 0, jnp.concatenate([taps, blank], axis=1), jnp.concatenate([blank, taps], axis=1))
    r["q0"][...] = jnp.concatenate([squares, taps], axis=0)
    part = nn((wide * r["gain"][...]).astype(BF16), r["down"][...]).astype(BF16)
    for g in groups_in:
        g["p"][...] = part[:, g["cols"]].reshape(g["p"].shape)
    share = x * ncore + core
    half = r["state_w"].shape[0]
    span = rank // (nx * ncore)
    loads["state_w"].wait()
    gz = r["gz"]
    gz[z] = r["state_w"][:, pl.ds(pl.multiple_of(share * span, span), span)]
    pl.semaphore_wait(barrier, len(peers))

    picked = z // 2
    held = {}
    nothing = lambda: None

    def hook0():
        held["q"] = cp.go(r["q0"], r["q1"], yl=other)
        held["gz"] = []
        for o in range(1, nz):
            copy = cp.make(gz.at[z], gz.at[z], z=at(o))
            cp.all.pop()
            sends = at(o) // 2 == lax.rem(z, 4)
            comes = lax.rem(at(-o), 4) == picked
            held["gz"].append((sends, comes, copy))

            @pl.when(sends)
            def _():
                copy.start()

    def hook1():
        held["q"].wait_recv()
        r["qz"][z] = r["q0"][...] + r["q1"][...]
        held["qz"] = [cp.go(r["qz"].at[z], r["qz"].at[z], z=at(o)) for o in range(1, nz)]

    def hook2():
        for sends, comes, copy in held["gz"]:
            @pl.when(comes)
            def _():
                copy.wait_recv()

            @pl.when(sends)
            def _():
                copy.wait_send()

        for k in range(2):
            r["ss"][share, k, y] = gz[4 * k + picked]
        held["ss"] = cp.go(r["ss"].at[share, :, y], r["ss"].at[share, :, y], yl=other)

    def hook3():
        held["ss"].wait_recv()
        held["shares"] = [cp.go(r["ss"].at[share], r["ss"].at[share], **share_peer(o, c)) for o, c in shares]

    fac = r["fac"]

    def factor():
        if "factor" not in held:
            held["factor"] = True
            for copy in held["qz"]:
                copy.wait_recv()
            summed = r["qz"][0]
            for k in range(1, nz):
                summed = summed + r["qz"][k]
            near = 2 * rows
            per = 128 // near
            row = jnp.zeros((1, 128), F32)
            for c in range(tokens // 128):
                row = jnp.where(z // per == c, summed[c : c + 1], row)
            wanted = lax.broadcasted_iota(jnp.int32, (near, 128), 1) == lax.broadcasted_iota(jnp.int32, (near, 128), 0) + near * lax.rem(z, per)
            mean = jnp.sum(jnp.where(wanted, row, 0.0), axis=1, keepdims=True) / (width * nz * nyl)
            fac[...] = jnp.broadcast_to(lax.rsqrt(mean + EPS), (near, 128)).reshape(2, rows, 128)
        return Column(fac)

    flows = [FLOWS[g["order"]](cp, env, g, None, factor, nothing) for g in groups_in]
    for flow, g in zip(flows, groups_in):
        if g["order"] == "y":
            next(flow)
    run_flows(flows, (hook0, hook1, hook2, hook3))

    last = pl.ds(rows - 16, 16)
    following = seq_shift(sizes, place, 1)
    halos = [cp.go(g["g"].at[nz - 1, 1, last], g["halo"], **following) for g in groups_in]
    reds = [g["g"][...].reshape(tokens, -1) for g in groups_in]
    cuts = [g["cols"] for g in groups_in]
    over = lambda f, blocks, take: sum(f(b, take(c)) for b, c in zip(blocks, cuts))

    for copy in held["shares"]:
        copy.wait_recv()
    swt = r["swt"]
    for k in range(nx * ncore):
        swt[:, span * k : span * (k + 1)] = r["ss"][k].reshape(2 * nyl * half, span)
    pre = r["pre"]
    chans = 2 * nyl * half
    for name in ("value_w", "step_w", "gate_w"):
        loads[name].wait()
    value_w = r["value_w"]

    def project(blocks):
        return over(nn, blocks, lambda c: value_w[c]), over(nt, blocks, lambda c: swt[:, c])

    pre[16:, :width], pre[16:, width:] = project(reds)

    heads = r["step_w"].shape[0]
    step_t = jnp.concatenate([r["step_w"][...].astype(F32), jnp.zeros((8 - heads, rank), F32)], axis=0).astype(BF16)
    raw = over(lambda b, w: nt(w, b), reds, lambda c: step_t[:, c])
    head = lax.broadcasted_iota(jnp.int32, (8, 1), 0)
    bias, decay = jnp.zeros((8, 1), F32), jnp.zeros((8, 1), F32)
    for h in range(heads):
        bias = jnp.where(head == h, r["bias"][h], bias)
        decay = jnp.where(head == h, r["decay"][h], decay)
    raw = raw + bias
    step = jnp.maximum(raw, 0.0) + jnp.log1p(jnp.exp(-jnp.abs(raw)))
    lane = lax.broadcasted_iota(jnp.int32, (8, tokens), 1)
    logs = -jnp.exp(decay) * step
    k = 1
    while k < tokens:
        logs = logs + jnp.where(lane >= k, pltpu.roll(logs, k, axis=1), 0.0)
        k *= 2
    final = logs[:, tokens - 1 : tokens]
    ending = jnp.exp(final - logs) * step
    stack = jnp.concatenate([logs, ending, jnp.exp(logs), jnp.zeros((104, tokens), F32)], axis=0)
    cols = r["cols"]
    cols[...] = stack.T
    whole = jnp.exp(final)

    gates = over(nn, reds, lambda c: r["gate_w"][c])
    r["gact"][...] = silu(gates)
    vact, bact, cact = r["vact"], r["bact"], r["cact"]
    weights = r["conv_v"][...]
    sweights = jnp.concatenate([r["qz"][picked][4:8], r["qz"][4 + picked][4:8]], axis=1)

    def convolve(c):
        acc_v = jnp.zeros((128, width), F32)
        acc_s = jnp.zeros((128, chans), F32)
        for t in range(4):
            window = pre[13 + t + 128 * c : 13 + t + 128 * c + 128, :]
            acc_v = acc_v + weights[t : t + 1] * window[:, :width]
            acc_s = acc_s + sweights[t : t + 1] * window[:, width:]
        here = slice(128 * c, 128 * c + 128)
        vact[here] = silu(acc_v).astype(BF16)
        acts = silu(acc_s).astype(BF16)
        bact[here] = acts[:, :128]
        cact[here] = acts[:, 128:]

    for c in range(1, tokens // 128):
        convolve(c)
    for copy in halos:
        copy.wait_recv()
    hv, hs = project([g["halo"][...] for g in groups_in])
    keep = jnp.where(place == 0, 0.0, 1.0)
    pre[:16, :width] = hv * keep
    pre[:16, width:] = hs * keep
    convolve(0)

    eye = (lax.broadcasted_iota(jnp.int32, (128, 128), 0) == lax.broadcasted_iota(jnp.int32, (128, 128), 1)).astype(BF16)
    b_t = nt(eye, bact[...]).astype(BF16)
    own_state, own_decay = [], []
    for p in range(2):
        h = 2 * p
        ends = halves(cols[:, 8 + h : 9 + h], cols[:, 9 + h : 10 + h])
        scaled = (vact[:, 128 * p : 128 * p + 128].astype(F32) * ends).astype(BF16)
        own_state.append(nn(b_t, scaled))
        own_decay.append(halves(whole[h : h + 1], whole[h + 1 : h + 2]))
    theirs = lambda a, b, c: jnp.where(c == 0, a, b)
    one_send, one_recv = r["one"].at[0], r["one"].at[1]
    pack(r["one"], 0, theirs(*own_state, twin), theirs(*own_decay, twin))
    first = cp.go(one_send, one_recv, core=twin)
    mine, mine_decay = theirs(*own_state, core), theirs(*own_decay, core)
    first.wait_recv()
    got, got_decay = unpack(r["one"], 1)
    state0, state1 = jnp.where(core == 0, mine, got), jnp.where(core == 0, got, mine)
    decay0, decay1 = jnp.where(core == 0, mine_decay, got_decay), jnp.where(core == 0, got_decay, mine_decay)
    pack(r["two"], yh, decay1 * state0 + state1, decay0 * decay1)
    second = gather_scan(cp, r["two"], yh, nyh, "yh")

    mix = r["mix"]
    for c in range(tokens // 128):
        here = slice(128 * c, 128 * c + 128)
        past = 128 * c + 128
        couple = nt(cact[here], bact[:past])
        seen = lax.broadcasted_iota(jnp.int32, (128, past), 0) + 128 * c >= lax.broadcasted_iota(jnp.int32, (128, past), 1)
        for p in range(2):
            outs = []
            for h in (2 * p, 2 * p + 1):
                spread = cols[here, h : h + 1] - logs[h : h + 1, :past]
                fade = jnp.where(seen, jnp.exp(jnp.minimum(spread, 0.0)), 0.0)
                m = (couple * fade * step[h : h + 1, :past]).astype(BF16)
                outs.append(nn(m, vact[:past, 128 * p : 128 * p + 128]))
            skip = halves(jnp.full((1, 1), r["skip"][2 * p], F32), jnp.full((1, 1), r["skip"][2 * p + 1], F32))
            values = vact[here, 128 * p : 128 * p + 128].astype(F32)
            mix[here, 128 * p : 128 * p + 128] = halves(*outs) + skip * values

    for copy in second:
        copy.wait_recv()
    before, before_decay, run, run_decay = prefix(r["two"], yh, nyh)
    pack(r["three"], x, run, run_decay)
    third = gather_scan(cp, r["three"], x, nx, "x")
    for copy in third:
        copy.wait_recv()
    far = prefix(r["three"], x, nx)[0]
    entry0 = before_decay * far + before
    entry1 = decay0 * entry0 + state0
    inc = r["inc"]
    inc[core] = theirs(entry0, entry1, core).astype(BF16)
    r["fin"][...] = theirs(entry0, entry1, twin).astype(BF16)
    fourth = cp.go(r["fin"], inc.at[core], core=twin)
    fourth.wait_recv()

    gated = []
    for p in range(2):
        h = 2 * p
        carried = nn(cact[...], inc[p]) * halves(cols[:, 16 + h : 17 + h], cols[:, 17 + h : 18 + h])
        gated.append((mix[:, 128 * p : 128 * p + 128] + carried) * r["gact"][:, 128 * p : 128 * p + 128])
    gated = jnp.concatenate(gated, axis=1)
    high, low = split2(gated * gated)
    own = token_rows(nt(ones, high) + nt(ones, low))
    r["gq"][0] = jnp.concatenate([own, jnp.zeros_like(own)], axis=0)
    groups = [
        cp.go(r["gq"].at[0], r["gq"].at[1], yl=other),
        cp.go(r["gq"].at[0], r["gq"].at[2], z=mate),
        cp.go(r["gq"].at[0], r["gq"].at[3], z=mate, yl=other),
    ]
    loads["odown"].wait()
    pf = r["pf"]
    pf[...] = nn((gated * r["gain2"][...]).astype(BF16), r["odown"][...])
    nrm = r["nrm"]
    for g in groups_out:
        if g["order"] == "y":
            g["p"][...] = pf[:, g["cols"]].astype(BF16).reshape(g["p"].shape)
    early = [FLOWS["y"](cp, env, g, nrm, None, nothing) for g in groups_out if g["order"] == "y"]
    for flow in early + early:
        next(flow)
    for copy in groups:
        copy.wait_recv()
    squares = r["gq"][0] + r["gq"][1] + r["gq"][2] + r["gq"][3]
    norm = lax.rsqrt(squares / (width * 4) + EPS)
    norm = jnp.concatenate([norm, jnp.zeros((120, 128), F32)], axis=0).T
    per = 128 // (2 * rows)
    for c in range(tokens // 128):
        by_row = jnp.broadcast_to(norm[:, c : c + 1], (128, 128))
        nrm[per * c : per * c + per] = by_row.reshape(per, 2, rows, 128)
        for g in groups_out:
            if g["order"] == "z":
                scaled = (pf[128 * c : 128 * c + 128, g["cols"]] * by_row[:, :1]).astype(BF16)
                g["p"][per * c : per * c + per] = scaled.reshape(per, *g["p"].shape[1:])
    late = [FLOWS["z"](cp, env, g, None, None, nothing) for g in groups_out if g["order"] == "z"]
    for flow in late:
        next(flow)
    run_flows(late + early, ())
    loads["oup"].wait()
    oup = r["oup"]
    update = over(nn, [g["g"][...].reshape(tokens, -1) for g in groups_out], lambda c: oup[c])
    r["out"][...] = (hid[...].astype(F32) + update).astype(BF16)
    cp.drain()


def on_device(sizes, hidden, norm_gain, rank_down, gate_up, value_up, state_up, step_up, conv_value, conv_state, step_bias, decay_log, skip_gain, gate_gain, out_down, out_up):
    nx, nyh, ncore, nz, nyl = sizes
    tokens, width = hidden.shape
    rank = rank_down.shape[1]
    half = state_up.shape[1]
    rows = tokens // (nz * nyl)
    vm, hbm, sm = (pl.BlockSpec(memory_space=s) for s in (pltpu.VMEM, pl.ANY, pltpu.SMEM))
    operands = [
        ("hid_h", hbm, hidden), ("gain", vm, norm_gain.reshape(1, -1)), ("down_h", hbm, rank_down), ("gate_w_h", hbm, gate_up),
        ("value_w_h", hbm, value_up), ("state_w_h", hbm, state_up.T), ("step_w_h", hbm, step_up.T), ("conv_v", vm, conv_value),
        ("conv_s", vm, conv_state), ("bias", sm, step_bias), ("decay", sm, decay_log), ("skip", sm, skip_gain),
        ("gain2", vm, gate_gain.reshape(1, -1)), ("odown_h", hbm, out_down), ("oup_h", hbm, out_up),
    ]
    like = lambda a: pltpu.VMEM(a.shape, a.dtype)
    count = 400
    scratch = [
        ("hid", like(hidden)), ("down", like(rank_down)), ("gate_w", like(gate_up)), ("value_w", like(value_up)), ("state_w", like(state_up.T)),
        ("step_w", like(step_up.T)), ("odown", like(out_down)), ("oup", like(out_up)), *group_buffers("in", nz, rows), *group_buffers("out", nz, rows),
        ("q0", pltpu.VMEM((8, 128), F32)), ("q1", pltpu.VMEM((8, 128), F32)), ("qz", pltpu.VMEM((nz, 8, 128), F32)),
        ("gz", pltpu.VMEM((nz, half, rank // (nx * ncore)), BF16)), ("ss", pltpu.VMEM((nx * ncore, 2, nyl, half, rank // (nx * ncore)), BF16)),
        ("swt", pltpu.VMEM((2 * nyl * half, rank), BF16)), ("fac", pltpu.VMEM((2, rows, 128), F32)),
        ("pre", pltpu.VMEM((16 + tokens, width + 2 * nyl * half), F32)), ("vact", pltpu.VMEM((tokens, width), BF16)),
        ("bact", pltpu.VMEM((tokens, 128), BF16)), ("cact", pltpu.VMEM((tokens, 128), BF16)), ("gact", pltpu.VMEM((tokens, width), F32)),
        ("cols", pltpu.VMEM((tokens, 128), F32)), ("mix", pltpu.VMEM((tokens, width), F32)), ("pf", pltpu.VMEM((tokens, rank), F32)),
        ("nrm", pltpu.VMEM((nz, 2, rows, 128), F32)),
        ("one", pltpu.VMEM((2, 144, 128), BF16)), ("two", pltpu.VMEM((nyh, 144, 128), BF16)), ("three", pltpu.VMEM((nx, 144, 128), BF16)),
        ("fin", pltpu.VMEM((128, 128), BF16)), ("inc", pltpu.VMEM((2, 128, 128), BF16)), ("gq", pltpu.VMEM((4, 8, 128), F32)),
        ("send", pltpu.SemaphoreType.DMA((count,))), ("recv", pltpu.SemaphoreType.DMA((count,))), ("load_sem", pltpu.SemaphoreType.DMA((8,))),
    ]
    names = [n for n, _, _ in operands] + ["out"] + [n for n, _ in scratch]
    return pl.pallas_call(
        functools.partial(block_kernel, sizes, names),
        out_shape=jax.ShapeDtypeStruct(hidden.shape, BF16),
        in_specs=[s for _, s, _ in operands],
        out_specs=vm,
        scratch_shapes=[s for _, s in scratch],
        compiler_params=pltpu.CompilerParams(collective_id=0, has_side_effects=True, vmem_limit_bytes=60 * 2**20),
    )(*(a for _, _, a in operands))


def grid_sizes(mesh):
    seq, tp = mesh.shape["seq"], mesh.shape["tp"]
    nx = nyh = 1
    if seq == 32:
        nx = nyh = 4
    return (nx, nyh, 2, tp // 2, 2)


def solution(mesh):
    sizes = grid_sizes(mesh)
    finer = Mesh(mesh.devices.reshape(sizes), SEQ + TP)
    rows, cols, flat = P(TP, None), P(None, TP), P(TP)
    placed = (P(SEQ, TP), flat, rows, cols, cols, cols, cols, cols, cols, flat, flat, flat, flat, rows, cols)
    return jax.shard_map(
        functools.partial(on_device, sizes), mesh=finer, in_specs=placed, out_specs=P(SEQ, TP), check_vma=False
    )
```

```python
import functools

import jax
import jax.numpy as jnp
from jax import lax
from jax.experimental import pallas as pl
from jax.experimental.pallas import tpu as pltpu
from jax.sharding import Mesh
from jax.sharding import PartitionSpec as P

GROUPS = 4
EPS = 1e-05
SEQ = ("x", "yh", "core")
TP = ("z", "yl")
F32 = jnp.float32
BF16 = jnp.bfloat16
MESH = pl.DeviceIdType.MESH

ORDER = (3, -3, 4, 2, -2, 1, -1, 0)
SKIP = (True, True)
EARLY = 3
PARTS = (("y", 256), ("y", 256), ("y", 256), ("z", 256))


def nt(a, b):
    return lax.dot_general(a, b, (((1,), (1,)), ((), ())), preferred_element_type=F32)


def nn(a, b):
    return jnp.dot(a, b, preferred_element_type=F32)


def silu(x):
    return x * (1.0 / (1.0 + jnp.exp(-x)))


def split2(x):
    high = x.astype(BF16)
    return high, (x - high.astype(F32)).astype(BF16)


class Copies:
    def __init__(self, send, recv):
        self.send, self.recv, self.used, self.all = send, recv, 0, []

    def make(self, src, dst, **where):
        k = self.used
        self.used += 1
        copy = pltpu.make_async_remote_copy(
            src_ref=src,
            dst_ref=dst,
            send_sem=self.send.at[k],
            recv_sem=self.recv.at[k],
            device_id=where,
            device_id_type=MESH,
        )
        self.all.append(copy)
        return copy

    def go(self, src, dst, **where):
        copy = self.make(src, dst, **where)
        copy.start()
        return copy

    def drain(self):
        for copy in self.all:
            copy.wait_send()
        self.all = []


def up(v):
    return v.astype(F32)


def flow_y_first(cp, env, buf, scale, factor, done):
    z, y, nz = env
    at = lambda off: lax.rem(z + off + nz, nz)
    other = 1 - y
    p, yr, r, h, g = buf["p"], buf["y"], buf["r"], buf["h"], buf["g"]
    part = {1: pl.ds(0, 16), -1: pl.ds(16, 16)}
    across, got = {}, {}
    def cross(first, last):
        for k in range(first, last):
            off = ORDER[k]
            across[off] = (k, cp.go(p.at[at(off), other], yr.at[k], yl=other))

    cross(0, 3)
    yield
    cross(3, EARLY)
    yield

    def own(off):
        k, copy = across[off]
        copy.wait_recv()
        sums = up(p[at(off), y]) + up(yr[k])
        return sums if scale is None else sums * scale[at(off), y][:, :1]

    for d, s in ((0, 1), (1, -1)):
        p[at(3 * s), y] = own(3 * s).astype(BF16)
        got[s, 3] = cp.go(p.at[at(3 * s), y], r.at[d, 0], z=at(s))
    p[at(4), y] = own(4).astype(BF16)
    for s in (1, -1):
        got[s, 4] = cp.go(p.at[at(4), y, part[s]], h.at[part[s]], z=at(2 * s))
    cross(EARLY, len(ORDER))
    yield
    far = 2 if SKIP[0] else 1
    for d, s in ((0, 1), (1, -1)):
        mine = own(2 * s)
        got[s, 3].wait_recv()
        got[s, 4].wait_recv()
        r[d, 0] = (up(r[d, 0]) + mine).astype(BF16)
        r[d, 0, part[s]] = (up(r[d, 0, part[s]]) + up(h[part[s]])).astype(BF16)
        got[s, 2] = cp.go(r.at[d, 0], r.at[d, 1], z=at(far * s))
        if SKIP[0]:
            p[at(s), y] = own(s).astype(BF16)
            got[s, 1] = cp.go(p.at[at(s), y], r.at[d, 2], z=at(s))
    yield
    if not SKIP[0]:
        for d, s in ((0, 1), (1, -1)):
            mine = own(s)
            got[s, 2].wait_recv()
            r[d, 1] = (up(r[d, 1]) + mine).astype(BF16)
            got[s, 1] = cp.go(r.at[d, 1], r.at[d, 2], z=at(s))
        yield
    total = own(0)
    for d, s in ((0, 1), (1, -1)):
        for e in (1, 2) if SKIP[0] else (2,):
            got[s, 3 - e].wait_recv()
            total = total + up(r[d, e])
    if factor is not None:
        total = total * factor()[y]
    mine = g.at[z, y]
    g[z, y] = total.astype(BF16)
    seen = {}
    for hop in (1, 2) if SKIP[1] else (1,):
        for s in (1, -1):
            seen[s, hop] = cp.go(mine, mine, z=at(hop * s))
    last = [cp.go(mine, mine, yl=other)]
    yield
    for k in (1, 2, 3):
        for s in (1, -1):
            seen[s, k].wait_recv()
            block = g.at[at(-k * s), y]
            if k == 1 and not SKIP[1]:
                seen[s, 2] = cp.go(block, block, z=at(s))
            if k == 2:
                half = g.at[at(-2 * s), y, part[s]]
                seen[s, 4] = cp.go(half, half, z=at(2 * s))
                seen[s, 3] = cp.go(block, block, z=at(s))
            last.append(cp.go(block, block, yl=other))
        yield
    for s in (1, -1):
        seen[s, 4].wait_recv()
        half = g.at[at(4), y, part[s]]
        last.append(cp.go(half, half, yl=other))
    yield
    for copy in last:
        copy.wait_recv()
    done()


def flow_z_first(cp, env, buf, scale, factor, done):
    z, y, nz = env
    at = lambda off: lax.rem(z + off + nz, nz)
    p, yr, r, h, g = buf["p"], buf["y"], buf["r"], buf["h"], buf["g"]
    part = {1: pl.ds(0, 16), -1: pl.ds(16, 16)}
    every = slice(None)
    got, seen = {}, {}
    for d, s in ((0, 1), (1, -1)):
        got[s, 3] = cp.go(p.at[at(3 * s)], r.at[d, 0], z=at(s))
        got[s, 4] = cp.go(p.at[at(4), :, part[s]], h.at[:, part[s]], z=at(2 * s))
    if SKIP[0]:
        for d, s in ((0, 1), (1, -1)):
            got[s, 1] = cp.go(p.at[at(s)], r.at[d, 2], z=at(s))
    yield
    far = 2 if SKIP[0] else 1
    for d, s in ((0, 1), (1, -1)):
        got[s, 3].wait_recv()
        got[s, 4].wait_recv()
        r[d, 0] = (up(r[d, 0]) + up(p[at(2 * s)])).astype(BF16)
        r[d, 0, :, part[s]] = (up(r[d, 0, :, part[s]]) + up(h[:, part[s]])).astype(BF16)
        got[s, 2] = cp.go(r.at[d, 0], r.at[d, 1], z=at(far * s))
    yield
    if not SKIP[0]:
        for d, s in ((0, 1), (1, -1)):
            got[s, 2].wait_recv()
            r[d, 1] = (up(r[d, 1]) + up(p[at(s)])).astype(BF16)
            got[s, 1] = cp.go(r.at[d, 1], r.at[d, 2], z=at(s))
        yield
    total = up(p[z])
    for d, s in ((0, 1), (1, -1)):
        for e in (1, 2) if SKIP[0] else (2,):
            got[s, 3 - e].wait_recv()
            total = total + up(r[d, e])
    yr[0] = total.astype(BF16)
    swap = cp.go(yr.at[0], yr.at[1], yl=1 - y)
    yield
    swap.wait_recv()
    total = up(yr[0]) + up(yr[1])
    if factor is not None:
        total = total * factor()[...]
    g[z] = total.astype(BF16)
    for hop in (1, 2) if SKIP[1] else (1,):
        for s in (1, -1):
            seen[s, hop] = cp.go(g.at[z], g.at[z], z=at(hop * s))
    yield
    for k in (1, 2, 3):
        for s in (1, -1):
            seen[s, k].wait_recv()
            block = g.at[at(-k * s)]
            if k == 1 and not SKIP[1]:
                seen[s, 2] = cp.go(block, block, z=at(s))
            if k == 2:
                half = g.at[at(-2 * s), :, part[s]]
                seen[s, 4] = cp.go(half, half, z=at(2 * s))
                seen[s, 3] = cp.go(block, block, z=at(s))
        yield
    for s in (1, -1):
        seen[s, 4].wait_recv()
    done()


def run_flows(flows, hooks):
    turn = 0
    while flows:
        hooks[turn]() if turn < len(hooks) else None
        turn += 1
        left = []
        for flow in flows:
            if next(flow, flow) is not flow:
                left.append(flow)
        flows = left


def gather_scan(cp, buf, place, peers, axis):
    copies = []
    for o in sorted(range(1, peers), key=lambda o: -min(o, peers - o)):
        there = lax.rem(place + o, peers)
        copies.append(cp.go(buf.at[place], buf.at[place], **{axis: there}))
    return copies


def pack(ref, where, state, decay):
    high, low = split2(decay)
    ref[where, pl.ds(0, 128), :] = state.astype(BF16)
    row = lax.broadcasted_iota(jnp.int32, (16, 128), 0)
    tail = jnp.where(row == 0, high.astype(F32), jnp.where(row == 1, low.astype(F32), 0.0))
    ref[where, pl.ds(128, 16), :] = tail.astype(BF16)


def unpack(ref, where):
    tail = ref[where, pl.ds(128, 16), :].astype(F32)
    return ref[where, pl.ds(0, 128), :].astype(F32), tail[0:1] + tail[1:2]


def prefix(buf, place, peers):
    run, decay = jnp.zeros((128, 128), F32), jnp.ones((1, 128), F32)
    before, before_decay = run, decay
    for k in range(peers):
        here = place == k
        before = jnp.where(here, run, before)
        before_decay = jnp.where(here, decay, before_decay)
        state, d = unpack(buf, k)
        run, decay = d * run + state, d * decay
    return before, before_decay, run, decay


FLOWS = {"y": flow_y_first, "z": flow_z_first}


class Column:
    def __init__(self, ref):
        self.ref = ref

    def __getitem__(self, k):
        return self.ref[k][..., :1]


def group_buffers(side, nz, rows):
    out = []
    for i, (order, c) in enumerate(PARTS):
        both = (2, rows, c) if order == "z" else (rows, c)
        shapes = dict(p=(nz, 2, rows, c), g=(nz, 2, rows, c), r=(2, 3, *both), h=both, y=(2, *both) if order == "z" else (nz, *both))
        if side == "in":
            shapes["halo"] = (16, c)
        out += [(f"{side}{i}{k}", pltpu.VMEM(v, BF16)) for k, v in shapes.items()]
    return out


def split_groups(r, side):
    out, start = [], 0
    for i, (order, c) in enumerate(PARTS):
        g = {k: r[f"{side}{i}{k}"] for k in ("p", "g", "r", "h", "y", "halo") if f"{side}{i}{k}" in r}
        out.append(dict(g, order=order, cols=slice(start, start + c)))
        start += c
    return out


def seq_shift(sizes, place, by):
    nx, nyh, ncore = sizes[:3]
    total = nx * nyh * ncore
    there = lax.rem(place + by + total, total)
    return dict(x=there // (nyh * ncore), yh=lax.rem(there // ncore, nyh), core=lax.rem(there, ncore))


def token_rows(v):
    return jnp.concatenate([v[0:1, 128 * c : 128 * c + 128] for c in range(v.shape[1] // 128)], axis=0)


def halves(low, high):
    lane = lax.broadcasted_iota(jnp.int32, (low.shape[0], 128), 1)
    return jnp.where(lane < 64, low, high)


def block_kernel(sizes, names, *args):
    r = dict(zip(names, args))
    nx, nyh, ncore, nz, nyl = sizes
    x, yh, core, z, y = (lax.axis_index(a) for a in ("x", "yh", "core", "z", "yl"))
    other, twin = 1 - y, 1 - core
    hid, groups_in, groups_out = r["hid"], split_groups(r, "in"), split_groups(r, "out")
    tokens, width = hid.shape
    rows, rank = groups_in[0]["p"].shape[2], r["down"].shape[1]
    env = (z, y, nz)
    place = (x * nyh + yh) * ncore + core
    at = lambda off: lax.rem(z + off + nz, nz)
    mate = z + 1 - 2 * lax.rem(z, 2)
    cp = Copies(r["send"], r["recv"])

    shares = [(o, c) for o in range(nx) for c in range(ncore) if o or c]
    share_peer = lambda o, c: dict(x=lax.rem(x + o, nx), core=lax.rem(core + c, ncore))
    peers = [dict(z=at(o)) for o in range(1, nz)] + [dict(yl=other), dict(z=mate, yl=other)]
    peers += [dict(yh=lax.rem(yh + o, nyh)) for o in range(1, nyh)]
    peers += [share_peer(o, c) for o, c in shares]
    peers += [seq_shift(sizes, place, 1), seq_shift(sizes, place, -1)]
    barrier = pltpu.get_barrier_semaphore()
    for peer in peers:
        pl.semaphore_signal(barrier, inc=1, device_id=peer, device_id_type=MESH)

    loads = {}
    for k, name in enumerate(("hid", "down", "state_w", "value_w", "step_w", "gate_w", "odown", "oup")):
        loads[name] = pltpu.make_async_copy(r[name + "_h"], r[name], r["load_sem"].at[k])
        if k < 2:
            loads[name].start()

    loads["hid"].wait()
    loads["down"].wait()
    for name in ("state_w", "value_w", "step_w", "gate_w", "odown", "oup"):
        loads[name].start()
    wide = hid[...].astype(F32)
    ones = jnp.ones((8, width), BF16)
    high, low = split2(wide * wide)
    squares = token_rows(nt(ones, high) + nt(ones, low))
    taps = r["conv_s"][...]
    blank = jnp.zeros_like(taps)
    taps = jnp.where(y == 0, jnp.concatenate([taps, blank], axis=1), jnp.concatenate([blank, taps], axis=1))
    r["q0"][...] = jnp.concatenate([squares, taps], axis=0)
    part = nn((wide * r["gain"][...]).astype(BF16), r["down"][...]).astype(BF16)
    for g in groups_in:
        g["p"][...] = part[:, g["cols"]].reshape(g["p"].shape)
    share = x * ncore + core
    half = r["state_w"].shape[0]
    span = rank // (nx * ncore)
    loads["state_w"].wait()
    gz = r["gz"]
    gz[z] = r["state_w"][:, pl.ds(pl.multiple_of(share * span, span), span)]
    pl.semaphore_wait(barrier, len(peers))

    picked = z // 2
    held = {}
    nothing = lambda: None

    def hook0():
        held["q"] = cp.go(r["q0"], r["q1"], yl=other)
        held["gz"] = []
        for o in range(1, nz):
            copy = cp.make(gz.at[z], gz.at[z], z=at(o))
            cp.all.pop()
            sends = at(o) // 2 == lax.rem(z, 4)
            comes = lax.rem(at(-o), 4) == picked
            held["gz"].append((sends, comes, copy))

            @pl.when(sends)
            def _():
                copy.start()

    def hook1():
        held["q"].wait_recv()
        r["qz"][z] = r["q0"][...] + r["q1"][...]
        held["qz"] = [cp.go(r["qz"].at[z], r["qz"].at[z], z=at(o)) for o in range(1, nz)]

    def hook2():
        for sends, comes, copy in held["gz"]:
            @pl.when(comes)
            def _():
                copy.wait_recv()

            @pl.when(sends)
            def _():
                copy.wait_send()

        for k in range(2):
            r["ss"][share, k, y] = gz[4 * k + picked]
        held["ss"] = cp.go(r["ss"].at[share, :, y], r["ss"].at[share, :, y], yl=other)

    def hook3():
        held["ss"].wait_recv()
        held["shares"] = [cp.go(r["ss"].at[share], r["ss"].at[share], **share_peer(o, c)) for o, c in shares]

    fac = r["fac"]

    def factor():
        if "factor" not in held:
            held["factor"] = True
            for copy in held["qz"]:
                copy.wait_recv()
            summed = r["qz"][0]
            for k in range(1, nz):
                summed = summed + r["qz"][k]
            near = 2 * rows
            per = 128 // near
            row = jnp.zeros((1, 128), F32)
            for c in range(tokens // 128):
                row = jnp.where(z // per == c, summed[c : c + 1], row)
            wanted = lax.broadcasted_iota(jnp.int32, (near, 128), 1) == lax.broadcasted_iota(jnp.int32, (near, 128), 0) + near * lax.rem(z, per)
            mean = jnp.sum(jnp.where(wanted, row, 0.0), axis=1, keepdims=True) / (width * nz * nyl)
            fac[...] = jnp.broadcast_to(lax.rsqrt(mean + EPS), (near, 128)).reshape(2, rows, 128)
        return Column(fac)

    flows = {o: [FLOWS[o](cp, env, g, None, factor, nothing) for g in groups_in if g["order"] == o] for o in "zy"}
    for flow in flows["z"] + flows["y"] + flows["y"]:
        next(flow)
    run_flows(flows["y"] + flows["z"], (hook0, hook1, hook2, hook3))

    last = pl.ds(rows - 16, 16)
    following = seq_shift(sizes, place, 1)
    halos = [cp.go(g["g"].at[nz - 1, 1, last], g["halo"], **following) for g in groups_in]
    reds = [g["g"][...].reshape(tokens, -1) for g in groups_in]
    cuts = [g["cols"] for g in groups_in]
    over = lambda f, blocks, take: sum(f(b, take(c)) for b, c in zip(blocks, cuts))

    for copy in held["shares"]:
        copy.wait_recv()
    swt = r["swt"]
    for k in range(nx * ncore):
        swt[:, span * k : span * (k + 1)] = r["ss"][k].reshape(2 * nyl * half, span)
    pre = r["pre"]
    chans = 2 * nyl * half
    for name in ("value_w", "step_w", "gate_w"):
        loads[name].wait()
    value_w = r["value_w"]

    def project(blocks):
        return over(nn, blocks, lambda c: value_w[c]), over(nt, blocks, lambda c: swt[:, c])

    pre[16:, :width], pre[16:, width:] = project(reds)

    heads = r["step_w"].shape[0]
    step_t = jnp.concatenate([r["step_w"][...].astype(F32), jnp.zeros((8 - heads, rank), F32)], axis=0).astype(BF16)
    raw = over(lambda b, w: nt(w, b), reds, lambda c: step_t[:, c])
    head = lax.broadcasted_iota(jnp.int32, (8, 1), 0)
    bias, decay = jnp.zeros((8, 1), F32), jnp.zeros((8, 1), F32)
    for h in range(heads):
        bias = jnp.where(head == h, r["bias"][h], bias)
        decay = jnp.where(head == h, r["decay"][h], decay)
    raw = raw + bias
    step = jnp.maximum(raw, 0.0) + jnp.log1p(jnp.exp(-jnp.abs(raw)))
    lane = lax.broadcasted_iota(jnp.int32, (8, tokens), 1)
    logs = -jnp.exp(decay) * step
    k = 1
    while k < tokens:
        logs = logs + jnp.where(lane >= k, pltpu.roll(logs, k, axis=1), 0.0)
        k *= 2
    final = logs[:, tokens - 1 : tokens]
    ending = jnp.exp(final - logs) * step
    stack = jnp.concatenate([logs, ending, jnp.exp(logs), jnp.zeros((8, tokens), F32)], axis=0)
    cols = r["cols"]
    cols[...] = stack.T
    whole = jnp.exp(final)

    vact, bact, cact = r["vact"], r["bact"], r["cact"]
    weights = r["conv_v"][...]
    sweights = jnp.concatenate([r["qz"][picked][4:8], r["qz"][4 + picked][4:8]], axis=1)

    def convolve(c):
        acc_v = jnp.zeros((128, width), F32)
        acc_s = jnp.zeros((128, chans), F32)
        for t in range(4):
            window = pre[13 + t + 128 * c : 13 + t + 128 * c + 128, :]
            acc_v = acc_v + weights[t : t + 1] * window[:, :width]
            acc_s = acc_s + sweights[t : t + 1] * window[:, width:]
        here = slice(128 * c, 128 * c + 128)
        vact[here] = silu(acc_v).astype(BF16)
        acts = silu(acc_s).astype(BF16)
        bact[here] = acts[:, :128]
        cact[here] = acts[:, 128:]

    for c in range(1, tokens // 128):
        convolve(c)
    for copy in halos:
        copy.wait_recv()
    hv, hs = project([g["halo"][...] for g in groups_in])
    keep = jnp.where(place == 0, 0.0, 1.0)
    pre[:16, :width] = hv * keep
    pre[:16, width:] = hs * keep
    convolve(0)

    eye = (lax.broadcasted_iota(jnp.int32, (128, 128), 0) == lax.broadcasted_iota(jnp.int32, (128, 128), 1)).astype(BF16)
    b_t = nt(eye, bact[...]).astype(BF16)
    own_state, own_decay = [], []
    for p in range(2):
        h = 2 * p
        ends = halves(cols[:, 8 + h : 9 + h], cols[:, 9 + h : 10 + h])
        scaled = (vact[:, 128 * p : 128 * p + 128].astype(F32) * ends).astype(BF16)
        own_state.append(nn(b_t, scaled))
        own_decay.append(halves(whole[h : h + 1], whole[h + 1 : h + 2]))
    theirs = lambda a, b, c: jnp.where(c == 0, a, b)
    one_send, one_recv = r["one"].at[0], r["one"].at[1]
    pack(r["one"], 0, theirs(*own_state, twin), theirs(*own_decay, twin))
    first = cp.go(one_send, one_recv, core=twin)
    mine, mine_decay = theirs(*own_state, core), theirs(*own_decay, core)
    first.wait_recv()
    got, got_decay = unpack(r["one"], 1)
    state0, state1 = jnp.where(core == 0, mine, got), jnp.where(core == 0, got, mine)
    decay0, decay1 = jnp.where(core == 0, mine_decay, got_decay), jnp.where(core == 0, got_decay, mine_decay)
    pack(r["two"], yh, decay1 * state0 + state1, decay0 * decay1)
    second = gather_scan(cp, r["two"], yh, nyh, "yh")

    gates = over(nn, reds, lambda c: r["gate_w"][c])
    r["gact"][...] = silu(gates)
    mix = r["mix"]
    for c in range(tokens // 128):
        here = slice(128 * c, 128 * c + 128)
        past = 128 * c + 128
        couple = nt(cact[here], bact[:past])
        seen = lax.broadcasted_iota(jnp.int32, (128, past), 0) + 128 * c >= lax.broadcasted_iota(jnp.int32, (128, past), 1)
        for p in range(2):
            outs = []
            for h in (2 * p, 2 * p + 1):
                spread = cols[here, h : h + 1] - logs[h : h + 1, :past]
                fade = jnp.where(seen, jnp.exp(jnp.minimum(spread, 0.0)), 0.0)
                m = (couple * fade * step[h : h + 1, :past]).astype(BF16)
                outs.append(nn(m, vact[:past, 128 * p : 128 * p + 128]))
            skip = halves(jnp.full((1, 1), r["skip"][2 * p], F32), jnp.full((1, 1), r["skip"][2 * p + 1], F32))
            values = vact[here, 128 * p : 128 * p + 128].astype(F32)
            mix[here, 128 * p : 128 * p + 128] = halves(*outs) + skip * values

    for copy in second:
        copy.wait_recv()
    before, before_decay, run, run_decay = prefix(r["two"], yh, nyh)
    pack(r["three"], x, run, run_decay)
    third = gather_scan(cp, r["three"], x, nx, "x")
    for copy in third:
        copy.wait_recv()
    far = prefix(r["three"], x, nx)[0]
    entry0 = before_decay * far + before
    entry1 = decay0 * entry0 + state0
    inc = r["inc"]
    inc[core] = theirs(entry0, entry1, core).astype(BF16)
    r["fin"][...] = theirs(entry0, entry1, twin).astype(BF16)
    fourth = cp.go(r["fin"], inc.at[core], core=twin)
    fourth.wait_recv()

    gated = []
    for p in range(2):
        h = 2 * p
        carried = nn(cact[...], inc[p]) * halves(cols[:, 16 + h : 17 + h], cols[:, 17 + h : 18 + h])
        gated.append((mix[:, 128 * p : 128 * p + 128] + carried) * r["gact"][:, 128 * p : 128 * p + 128])
    gated = jnp.concatenate(gated, axis=1)
    high, low = split2(gated * gated)
    own = token_rows(nt(ones, high) + nt(ones, low))
    r["gq"][0] = jnp.concatenate([own, jnp.zeros_like(own)], axis=0)
    groups = [
        cp.go(r["gq"].at[0], r["gq"].at[1], yl=other),
        cp.go(r["gq"].at[0], r["gq"].at[2], z=mate),
        cp.go(r["gq"].at[0], r["gq"].at[3], z=mate, yl=other),
    ]
    loads["odown"].wait()
    pf = r["pf"]
    pf[...] = nn((gated * r["gain2"][...]).astype(BF16), r["odown"][...])
    nrm = r["nrm"]
    for g in groups_out:
        if g["order"] == "y":
            g["p"][...] = pf[:, g["cols"]].astype(BF16).reshape(g["p"].shape)
    early = [FLOWS["y"](cp, env, g, nrm, None, nothing) for g in groups_out if g["order"] == "y"]
    for flow in early:
        next(flow)
    for copy in groups:
        copy.wait_recv()
    squares = r["gq"][0] + r["gq"][1] + r["gq"][2] + r["gq"][3]
    norm = lax.rsqrt(squares / (width * 4) + EPS)
    norm = jnp.concatenate([norm, jnp.zeros((120, 128), F32)], axis=0).T
    per = 128 // (2 * rows)
    for c in range(tokens // 128):
        by_row = jnp.broadcast_to(norm[:, c : c + 1], (128, 128))
        nrm[per * c : per * c + per] = by_row.reshape(per, 2, rows, 128)
        for g in groups_out:
            if g["order"] == "z":
                scaled = (pf[128 * c : 128 * c + 128, g["cols"]] * by_row[:, :1]).astype(BF16)
                g["p"][per * c : per * c + per] = scaled.reshape(per, *g["p"].shape[1:])
    late = [FLOWS["z"](cp, env, g, None, None, nothing) for g in groups_out if g["order"] == "z"]
    for flow in late + early:
        next(flow)
    run_flows(early + late, ())
    loads["oup"].wait()
    oup = r["oup"]
    update = over(nn, [g["g"][...].reshape(tokens, -1) for g in groups_out], lambda c: oup[c])
    r["out"][...] = update
    cp.drain()


def on_device(sizes, hidden, norm_gain, rank_down, gate_up, value_up, state_up, step_up, conv_value, conv_state, step_bias, decay_log, skip_gain, gate_gain, out_down, out_up):
    nx, nyh, ncore, nz, nyl = sizes
    tokens, width = hidden.shape
    rank = rank_down.shape[1]
    half = state_up.shape[1]
    rows = tokens // (nz * nyl)
    vm, hbm, sm = (pl.BlockSpec(memory_space=s) for s in (pltpu.VMEM, pl.ANY, pltpu.SMEM))
    operands = [
        ("hid_h", hbm, hidden), ("gain", vm, norm_gain.reshape(1, -1)), ("down_h", hbm, rank_down), ("gate_w_h", hbm, gate_up),
        ("value_w_h", hbm, value_up), ("state_w_h", hbm, state_up.T), ("step_w_h", hbm, step_up.T), ("conv_v", vm, conv_value),
        ("conv_s", vm, conv_state), ("bias", sm, step_bias), ("decay", sm, decay_log), ("skip", sm, skip_gain),
        ("gain2", vm, gate_gain.reshape(1, -1)), ("odown_h", hbm, out_down), ("oup_h", hbm, out_up),
    ]
    like = lambda a: pltpu.VMEM(a.shape, a.dtype)
    count = 400
    scratch = [
        ("hid", like(hidden)), ("down", like(rank_down)), ("gate_w", like(gate_up)), ("value_w", like(value_up)), ("state_w", like(state_up.T)),
        ("step_w", like(step_up.T)), ("odown", like(out_down)), ("oup", like(out_up)), *group_buffers("in", nz, rows), *group_buffers("out", nz, rows),
        ("q0", pltpu.VMEM((8, 128), F32)), ("q1", pltpu.VMEM((8, 128), F32)), ("qz", pltpu.VMEM((nz, 8, 128), F32)),
        ("gz", pltpu.VMEM((nz, half, rank // (nx * ncore)), BF16)), ("ss", pltpu.VMEM((nx * ncore, 2, nyl, half, rank // (nx * ncore)), BF16)),
        ("swt", pltpu.VMEM((2 * nyl * half, rank), BF16)), ("fac", pltpu.VMEM((2, rows, 128), F32)),
        ("pre", pltpu.VMEM((16 + tokens, width + 2 * nyl * half), F32)), ("vact", pltpu.VMEM((tokens, width), BF16)),
        ("bact", pltpu.VMEM((tokens, 128), BF16)), ("cact", pltpu.VMEM((tokens, 128), BF16)), ("gact", pltpu.VMEM((tokens, width), F32)),
        ("cols", pltpu.VMEM((tokens, 32), F32)), ("mix", pltpu.VMEM((tokens, width), F32)), ("pf", pltpu.VMEM((tokens, rank), F32)),
        ("nrm", pltpu.VMEM((nz, 2, rows, 128), F32)),
        ("one", pltpu.VMEM((2, 144, 128), BF16)), ("two", pltpu.VMEM((nyh, 144, 128), BF16)), ("three", pltpu.VMEM((nx, 144, 128), BF16)),
        ("fin", pltpu.VMEM((128, 128), BF16)), ("inc", pltpu.VMEM((2, 128, 128), BF16)), ("gq", pltpu.VMEM((4, 8, 128), F32)),
        ("send", pltpu.SemaphoreType.DMA((count,))), ("recv", pltpu.SemaphoreType.DMA((count,))), ("load_sem", pltpu.SemaphoreType.DMA((8,))),
    ]
    names = [n for n, _, _ in operands] + ["out"] + [n for n, _ in scratch]
    update = pl.pallas_call(
        functools.partial(block_kernel, sizes, names),
        out_shape=jax.ShapeDtypeStruct(hidden.shape, F32),
        in_specs=[s for _, s, _ in operands],
        out_specs=vm,
        scratch_shapes=[s for _, s in scratch],
        compiler_params=pltpu.CompilerParams(collective_id=0, has_side_effects=True, vmem_limit_bytes=60 * 2**20),
    )(*(a for _, _, a in operands))
    return (hidden.astype(F32) + update).astype(BF16)


def grid_sizes(mesh):
    seq, tp = mesh.shape["seq"], mesh.shape["tp"]
    nx = nyh = 1
    if seq == 32:
        nx = nyh = 4
    return (nx, nyh, 2, tp // 2, 2)


def solution(mesh):
    sizes = grid_sizes(mesh)
    finer = Mesh(mesh.devices.reshape(sizes), SEQ + TP)
    rows, cols, flat = P(TP, None), P(None, TP), P(TP)
    placed = (P(SEQ, TP), flat, rows, cols, cols, cols, cols, cols, cols, flat, flat, flat, flat, rows, cols)
    return jax.shard_map(
        functools.partial(on_device, sizes), mesh=finer, in_specs=placed, out_specs=P(SEQ, TP), check_vma=False
    )
```

```python
import functools

import jax
import jax.numpy as jnp
from jax import lax
from jax.experimental import pallas as pl
from jax.experimental.pallas import tpu as pltpu
from jax.sharding import Mesh
from jax.sharding import PartitionSpec as P

GROUPS = 4
EPS = 1e-05
SEQ = ("x", "yh", "core")
TP = ("z", "yl")
F32 = jnp.float32
BF16 = jnp.bfloat16
MESH = pl.DeviceIdType.MESH

ORDER = (3, -3, 4, 2, -2, 1, -1, 0)
SKIP = (True, True)
SKIP_Z = (True, True)
EARLY = 3
PARTS = (("y", 256), ("y", 256), ("y", 256), ("z", 256))


def nt(a, b):
    return lax.dot_general(a, b, (((1,), (1,)), ((), ())), preferred_element_type=F32)


def nn(a, b):
    return jnp.dot(a, b, preferred_element_type=F32)


def silu(x):
    return x * (1.0 / (1.0 + jnp.exp(-x)))


def split2(x):
    high = x.astype(BF16)
    return high, (x - high.astype(F32)).astype(BF16)


class Copies:
    def __init__(self, send, recv):
        self.send, self.recv, self.sent, self.used = send, recv, 0, 0
        self.free, self.all, self.old = [], [], []

    def hold(self, src, dst, **where):
        if self.free:
            self.slot = self.free.pop()
        else:
            self.slot, self.sent = self.sent, self.sent + 1
        self.used += 1
        return pltpu.make_async_remote_copy(
            src_ref=src,
            dst_ref=dst,
            send_sem=self.send.at[self.slot],
            recv_sem=self.recv.at[self.used - 1],
            device_id=where,
            device_id_type=MESH,
        )

    def go(self, src, dst, **where):
        copy = self.hold(src, dst, **where)
        copy.start()
        self.all.append((copy, self.slot))
        return copy

    def turn(self):
        for copy, slot in self.old:
            copy.wait_send()
            self.free.append(slot)
        self.old, self.all = self.all, []

    def drain(self):
        self.turn()
        self.turn()


def up(v):
    return v.astype(F32)


def flow_y_first(cp, env, buf, scale, factor, done):
    z, y, nz = env
    at = lambda off: lax.rem(z + off + nz, nz)
    other = 1 - y
    p, yr, r, h, g = buf["p"], buf["y"], buf["r"], buf["h"], buf["g"]
    part = {1: pl.ds(0, 16), -1: pl.ds(16, 16)}
    across, got = {}, {}
    def cross(first, last):
        for k in range(first, last):
            off = ORDER[k]
            across[off] = (k, cp.go(p.at[at(off), other], yr.at[k], yl=other))

    cross(0, 3)
    yield
    cross(3, EARLY)
    yield

    def own(off):
        k, copy = across[off]
        copy.wait_recv()
        sums = up(p[at(off), y]) + up(yr[k])
        return sums if scale is None else sums * scale[at(off), y][:, :1]

    for d, s in ((0, 1), (1, -1)):
        p[at(3 * s), y] = own(3 * s).astype(BF16)
        got[s, 3] = cp.go(p.at[at(3 * s), y], r.at[d, 0], z=at(s))
    p[at(4), y] = own(4).astype(BF16)
    for s in (1, -1):
        got[s, 4] = cp.go(p.at[at(4), y, part[s]], h.at[part[s]], z=at(2 * s))
    cross(EARLY, len(ORDER))
    yield
    far = 2 if SKIP[0] else 1
    for d, s in ((0, 1), (1, -1)):
        mine = own(2 * s)
        got[s, 3].wait_recv()
        got[s, 4].wait_recv()
        r[d, 0] = (up(r[d, 0]) + mine).astype(BF16)
        r[d, 0, part[s]] = (up(r[d, 0, part[s]]) + up(h[part[s]])).astype(BF16)
        got[s, 2] = cp.go(r.at[d, 0], r.at[d, 1], z=at(far * s))
        if SKIP[0]:
            p[at(s), y] = own(s).astype(BF16)
            got[s, 1] = cp.go(p.at[at(s), y], r.at[d, 2], z=at(s))
    yield
    if not SKIP[0]:
        for d, s in ((0, 1), (1, -1)):
            mine = own(s)
            got[s, 2].wait_recv()
            r[d, 1] = (up(r[d, 1]) + mine).astype(BF16)
            got[s, 1] = cp.go(r.at[d, 1], r.at[d, 2], z=at(s))
        yield
    total = own(0)
    for d, s in ((0, 1), (1, -1)):
        for e in (1, 2) if SKIP[0] else (2,):
            got[s, 3 - e].wait_recv()
            total = total + up(r[d, e])
    if factor is not None:
        total = total * factor()[y]
    mine = g.at[z, y]
    g[z, y] = total.astype(BF16)
    seen = {}
    for hop in (1, 2) if SKIP[1] else (1,):
        for s in (1, -1):
            seen[s, hop] = cp.go(mine, mine, z=at(hop * s))
    last = [cp.go(mine, mine, yl=other)]
    yield
    for k in (1, 2, 3):
        for s in (1, -1):
            seen[s, k].wait_recv()
            block = g.at[at(-k * s), y]
            if k == 1 and not SKIP[1]:
                seen[s, 2] = cp.go(block, block, z=at(s))
            if k == 2:
                half = g.at[at(-2 * s), y, part[s]]
                seen[s, 4] = cp.go(half, half, z=at(2 * s))
                seen[s, 3] = cp.go(block, block, z=at(s))
            last.append(cp.go(block, block, yl=other))
        yield
    for s in (1, -1):
        seen[s, 4].wait_recv()
        half = g.at[at(4), y, part[s]]
        last.append(cp.go(half, half, yl=other))
    yield
    for copy in last:
        copy.wait_recv()
    done()


def flow_z_first(cp, env, buf, scale, factor, done):
    z, y, nz = env
    at = lambda off: lax.rem(z + off + nz, nz)
    p, yr, r, h, g = buf["p"], buf["y"], buf["r"], buf["h"], buf["g"]
    part = {1: pl.ds(0, 16), -1: pl.ds(16, 16)}
    every = slice(None)
    got, seen = {}, {}
    for d, s in ((0, 1), (1, -1)):
        got[s, 4] = cp.go(p.at[at(4), :, part[s]], h.at[:, part[s]], z=at(2 * s))
        got[s, 3] = cp.go(p.at[at(3 * s)], r.at[d, 0], z=at(s))
    if SKIP_Z[0]:
        for d, s in ((0, 1), (1, -1)):
            got[s, 1] = cp.go(p.at[at(s)], r.at[d, 2], z=at(s))
    yield
    far = 2 if SKIP_Z[0] else 1
    for d, s in ((0, 1), (1, -1)):
        got[s, 3].wait_recv()
        got[s, 4].wait_recv()
        r[d, 0] = (up(r[d, 0]) + up(p[at(2 * s)])).astype(BF16)
        r[d, 0, :, part[s]] = (up(r[d, 0, :, part[s]]) + up(h[:, part[s]])).astype(BF16)
        got[s, 2] = cp.go(r.at[d, 0], r.at[d, 1], z=at(far * s))
    yield
    if not SKIP_Z[0]:
        for d, s in ((0, 1), (1, -1)):
            got[s, 2].wait_recv()
            r[d, 1] = (up(r[d, 1]) + up(p[at(s)])).astype(BF16)
            got[s, 1] = cp.go(r.at[d, 1], r.at[d, 2], z=at(s))
        yield
    total = up(p[z])
    for d, s in ((0, 1), (1, -1)):
        for e in (1, 2) if SKIP_Z[0] else (2,):
            got[s, 3 - e].wait_recv()
            total = total + up(r[d, e])
    yr[0] = total.astype(BF16)
    swap = cp.go(yr.at[0], yr.at[1], yl=1 - y)
    yield
    swap.wait_recv()
    total = up(yr[0]) + up(yr[1])
    if factor is not None:
        total = total * factor()[...]
    g[z] = total.astype(BF16)
    for hop in (1, 2) if SKIP_Z[1] else (1,):
        for s in (1, -1):
            seen[s, hop] = cp.go(g.at[z], g.at[z], z=at(hop * s))
    yield
    for k in (1, 2, 3):
        for s in (1, -1):
            seen[s, k].wait_recv()
            block = g.at[at(-k * s)]
            if k == 1 and not SKIP_Z[1]:
                seen[s, 2] = cp.go(block, block, z=at(s))
            if k == 2:
                half = g.at[at(-2 * s), :, part[s]]
                seen[s, 4] = cp.go(half, half, z=at(2 * s))
                seen[s, 3] = cp.go(block, block, z=at(s))
        yield
    for s in (1, -1):
        seen[s, 4].wait_recv()
    done()


def run_flows(cp, flows, hooks):
    turn = 0
    while flows:
        cp.turn()
        hooks[turn]() if turn < len(hooks) else None
        turn += 1
        left = []
        for flow in flows:
            if next(flow, flow) is not flow:
                left.append(flow)
        flows = left


def gather_scan(cp, buf, place, peers, axis):
    copies = []
    for o in sorted(range(1, peers), key=lambda o: -min(o, peers - o)):
        there = lax.rem(place + o, peers)
        copies.append(cp.go(buf.at[place], buf.at[place], **{axis: there}))
    return copies


def pack(ref, where, state, decay):
    high, low = split2(decay)
    ref[where, pl.ds(0, 128), :] = state.astype(BF16)
    row = lax.broadcasted_iota(jnp.int32, (16, 128), 0)
    tail = jnp.where(row == 0, high.astype(F32), jnp.where(row == 1, low.astype(F32), 0.0))
    ref[where, pl.ds(128, 16), :] = tail.astype(BF16)


def unpack(ref, where):
    tail = ref[where, pl.ds(128, 16), :].astype(F32)
    return ref[where, pl.ds(0, 128), :].astype(F32), tail[0:1] + tail[1:2]


def prefix(buf, place, peers):
    run, decay = jnp.zeros((128, 128), F32), jnp.ones((1, 128), F32)
    before, before_decay = run, decay
    for k in range(peers):
        here = place == k
        before = jnp.where(here, run, before)
        before_decay = jnp.where(here, decay, before_decay)
        state, d = unpack(buf, k)
        run, decay = d * run + state, d * decay
    return before, before_decay, run, decay


FLOWS = {"y": flow_y_first, "z": flow_z_first}


class Column:
    def __init__(self, ref):
        self.ref = ref

    def __getitem__(self, k):
        return self.ref[k][..., :1]


def group_buffers(side, nz, rows):
    out = []
    for i, (order, c) in enumerate(PARTS):
        both = (2, rows, c) if order == "z" else (rows, c)
        shapes = dict(p=(nz, 2, rows, c), g=(nz, 2, rows, c), r=(2, 3, *both), h=both, y=(2, *both) if order == "z" else (nz, *both))
        if side == "in":
            shapes["halo"] = (16, c)
        out += [(f"{side}{i}{k}", pltpu.VMEM(v, BF16)) for k, v in shapes.items()]
    return out


def split_groups(r, side):
    out, start = [], 0
    for i, (order, c) in enumerate(PARTS):
        g = {k: r[f"{side}{i}{k}"] for k in ("p", "g", "r", "h", "y", "halo") if f"{side}{i}{k}" in r}
        out.append(dict(g, order=order, cols=slice(start, start + c)))
        start += c
    return out


def seq_shift(sizes, place, by):
    nx, nyh, ncore = sizes[:3]
    total = nx * nyh * ncore
    there = lax.rem(place + by + total, total)
    return dict(x=there // (nyh * ncore), yh=lax.rem(there // ncore, nyh), core=lax.rem(there, ncore))


def token_rows(v):
    return jnp.concatenate([v[0:1, 128 * c : 128 * c + 128] for c in range(v.shape[1] // 128)], axis=0)


def halves(low, high):
    lane = lax.broadcasted_iota(jnp.int32, (low.shape[0], 128), 1)
    return jnp.where(lane < 64, low, high)


def block_kernel(sizes, names, *args):
    r = dict(zip(names, args))
    nx, nyh, ncore, nz, nyl = sizes
    x, yh, core, z, y = (lax.axis_index(a) for a in ("x", "yh", "core", "z", "yl"))
    other, twin = 1 - y, 1 - core
    hid, groups_in, groups_out = r["hid"], split_groups(r, "in"), split_groups(r, "out")
    tokens, width = hid.shape
    rows, rank = groups_in[0]["p"].shape[2], r["down"].shape[1]
    env = (z, y, nz)
    place = (x * nyh + yh) * ncore + core
    at = lambda off: lax.rem(z + off + nz, nz)
    mate = z + 1 - 2 * lax.rem(z, 2)
    cp = Copies(r["send"], r["recv"])

    shares = [(o, c) for o in range(nx) for c in range(ncore) if o or c]
    share_peer = lambda o, c: dict(x=lax.rem(x + o, nx), core=lax.rem(core + c, ncore))
    peers = [dict(z=at(o)) for o in range(1, nz)] + [dict(yl=other), dict(z=mate, yl=other)]
    peers += [dict(yh=lax.rem(yh + o, nyh)) for o in range(1, nyh)]
    peers += [share_peer(o, c) for o, c in shares]
    peers += [seq_shift(sizes, place, 1), seq_shift(sizes, place, -1)]
    barrier = pltpu.get_barrier_semaphore()
    for peer in peers:
        pl.semaphore_signal(barrier, inc=1, device_id=peer, device_id_type=MESH)

    loads = {}
    for k, name in enumerate(("hid", "down", "state_w", "value_w", "step_w", "gate_w", "odown", "oup")):
        loads[name] = pltpu.make_async_copy(r[name + "_h"], r[name], r["load_sem"].at[k])
        if k < 2:
            loads[name].start()

    loads["hid"].wait()
    loads["down"].wait()
    for name in ("state_w", "value_w", "step_w", "gate_w", "odown", "oup"):
        loads[name].start()
    wide = hid[...].astype(F32)
    ones = jnp.ones((8, width), BF16)
    high, low = split2(wide * wide)
    squares = token_rows(nt(ones, high) + nt(ones, low))
    taps = r["conv_s"][...]
    blank = jnp.zeros_like(taps)
    taps = jnp.where(y == 0, jnp.concatenate([taps, blank], axis=1), jnp.concatenate([blank, taps], axis=1))
    r["q0"][...] = jnp.concatenate([squares, taps], axis=0)
    part = nn((wide * r["gain"][...]).astype(BF16), r["down"][...]).astype(BF16)
    for g in groups_in:
        g["p"][...] = part[:, g["cols"]].reshape(g["p"].shape)
    share = x * ncore + core
    half = r["state_w"].shape[0]
    span = rank // (nx * ncore)
    loads["state_w"].wait()
    gz = r["gz"]
    gz[z] = r["state_w"][:, pl.ds(pl.multiple_of(share * span, span), span)]
    pl.semaphore_wait(barrier, len(peers))

    picked = z // 2
    held = {}
    nothing = lambda: None

    def hook0():
        held["q"] = cp.go(r["q0"], r["q1"], yl=other)
        held["gz"] = []
        for o in range(1, nz):
            copy = cp.hold(gz.at[z], gz.at[z], z=at(o))
            sends = at(o) // 2 == lax.rem(z, 4)
            comes = lax.rem(at(-o), 4) == picked
            held["gz"].append((sends, comes, copy))

            @pl.when(sends)
            def _():
                copy.start()

    def hook1():
        held["q"].wait_recv()
        r["qz"][z] = r["q0"][...] + r["q1"][...]
        held["qz"] = [cp.go(r["qz"].at[z], r["qz"].at[z], z=at(o)) for o in range(1, nz)]

    def hook2():
        for sends, comes, copy in held["gz"]:
            @pl.when(comes)
            def _():
                copy.wait_recv()

            @pl.when(sends)
            def _():
                copy.wait_send()

        for k in range(2):
            r["ss"][share, k, y] = gz[4 * k + picked]
        held["ss"] = cp.go(r["ss"].at[share, :, y], r["ss"].at[share, :, y], yl=other)

    def hook3():
        held["ss"].wait_recv()
        held["shares"] = [cp.go(r["ss"].at[share], r["ss"].at[share], **share_peer(o, c)) for o, c in shares]

    fac = r["fac"]

    def factor():
        if "factor" not in held:
            held["factor"] = True
            for copy in held["qz"]:
                copy.wait_recv()
            summed = r["qz"][0]
            for k in range(1, nz):
                summed = summed + r["qz"][k]
            near = 2 * rows
            per = 128 // near
            row = jnp.zeros((1, 128), F32)
            for c in range(tokens // 128):
                row = jnp.where(z // per == c, summed[c : c + 1], row)
            wanted = lax.broadcasted_iota(jnp.int32, (near, 128), 1) == lax.broadcasted_iota(jnp.int32, (near, 128), 0) + near * lax.rem(z, per)
            mean = jnp.sum(jnp.where(wanted, row, 0.0), axis=1, keepdims=True) / (width * nz * nyl)
            fac[...] = jnp.broadcast_to(lax.rsqrt(mean + EPS), (near, 128)).reshape(2, rows, 128)
        return Column(fac)

    value_w = r["value_w"]
    pre = r["pre"]
    gact = r["gact"]

    def begin(g):
        block = g["g"][...].reshape(tokens, -1)
        if "begun" not in held:
            held["begun"] = True
            for name in ("value_w", "step_w", "gate_w"):
                loads[name].wait()
            pre[16:, :width] = nn(block, value_w[g["cols"]])
        else:
            pre[16:, :width] += nn(block, value_w[g["cols"]])

    flows = {o: [FLOWS[o](cp, env, g, None, factor, functools.partial(begin, g) if o == "z" else nothing) for g in groups_in if g["order"] == o] for o in "zy"}
    for flow in flows["z"] + flows["y"] + flows["y"]:
        next(flow)
    run_flows(cp, flows["y"] + flows["z"], (hook0, hook1, hook2, hook3))

    last = pl.ds(rows - 16, 16)
    following = seq_shift(sizes, place, 1)
    halos = [cp.go(g["g"].at[nz - 1, 1, last], g["halo"], **following) for g in groups_in]
    reds = [g["g"][...].reshape(tokens, -1) for g in groups_in]
    cuts = [g["cols"] for g in groups_in]
    over = lambda f, blocks, take: sum(f(b, take(c)) for b, c in zip(blocks, cuts))

    for copy in held["shares"]:
        copy.wait_recv()
    swt = r["swt"]
    for k in range(nx * ncore):
        swt[:, span * k : span * (k + 1)] = r["ss"][k].reshape(2 * nyl * half, span)
    pre = r["pre"]
    chans = 2 * nyl * half
    value_w = r["value_w"]

    def project(blocks):
        return over(nn, blocks, lambda c: value_w[c]), over(nt, blocks, lambda c: swt[:, c])

    pre[16:, :width] += sum(nn(b, value_w[g["cols"]]) for b, g in zip(reds, groups_in) if g["order"] == "y")
    pre[16:, width:] = over(nt, reds, lambda c: swt[:, c])

    heads = r["step_w"].shape[0]
    step_t = jnp.concatenate([r["step_w"][...].astype(F32), jnp.zeros((8 - heads, rank), F32)], axis=0).astype(BF16)
    raw = over(lambda b, w: nt(w, b), reds, lambda c: step_t[:, c])
    head = lax.broadcasted_iota(jnp.int32, (8, 1), 0)
    bias, decay = jnp.zeros((8, 1), F32), jnp.zeros((8, 1), F32)
    for h in range(heads):
        bias = jnp.where(head == h, r["bias"][h], bias)
        decay = jnp.where(head == h, r["decay"][h], decay)
    raw = raw + bias
    step = jnp.maximum(raw, 0.0) + jnp.log1p(jnp.exp(-jnp.abs(raw)))
    lane = lax.broadcasted_iota(jnp.int32, (8, tokens), 1)
    logs = -jnp.exp(decay) * step
    k = 1
    while k < tokens:
        logs = logs + jnp.where(lane >= k, pltpu.roll(logs, k, axis=1), 0.0)
        k *= 2
    final = logs[:, tokens - 1 : tokens]
    ending = jnp.exp(final - logs) * step
    stack = jnp.concatenate([logs, ending, jnp.exp(logs), jnp.zeros((8, tokens), F32)], axis=0)
    cols = r["cols"]
    cols[...] = stack.T
    whole = jnp.exp(final)

    vact, bact, cact = r["vact"], r["bact"], r["cact"]
    weights = r["conv_v"][...]
    sweights = jnp.concatenate([r["qz"][picked][4:8], r["qz"][4 + picked][4:8]], axis=1)

    def convolve(c):
        acc_v = jnp.zeros((128, width), F32)
        acc_s = jnp.zeros((128, chans), F32)
        for t in range(4):
            window = pre[13 + t + 128 * c : 13 + t + 128 * c + 128, :]
            acc_v = acc_v + weights[t : t + 1] * window[:, :width]
            acc_s = acc_s + sweights[t : t + 1] * window[:, width:]
        here = slice(128 * c, 128 * c + 128)
        vact[here] = silu(acc_v).astype(BF16)
        acts = silu(acc_s).astype(BF16)
        bact[here] = acts[:, :128]
        cact[here] = acts[:, 128:]

    for c in range(1, tokens // 128):
        convolve(c)
    for copy in halos:
        copy.wait_recv()
    hv, hs = project([g["halo"][...] for g in groups_in])
    keep = jnp.where(place == 0, 0.0, 1.0)
    pre[:16, :width] = hv * keep
    pre[:16, width:] = hs * keep
    convolve(0)

    eye = (lax.broadcasted_iota(jnp.int32, (128, 128), 0) == lax.broadcasted_iota(jnp.int32, (128, 128), 1)).astype(BF16)
    b_t = nt(eye, bact[...]).astype(BF16)
    own_state, own_decay = [], []
    for p in range(2):
        h = 2 * p
        ends = halves(cols[:, 8 + h : 9 + h], cols[:, 9 + h : 10 + h])
        scaled = (vact[:, 128 * p : 128 * p + 128].astype(F32) * ends).astype(BF16)
        own_state.append(nn(b_t, scaled))
        own_decay.append(halves(whole[h : h + 1], whole[h + 1 : h + 2]))
    theirs = lambda a, b, c: jnp.where(c == 0, a, b)
    one_send, one_recv = r["one"].at[0], r["one"].at[1]
    pack(r["one"], 0, theirs(*own_state, twin), theirs(*own_decay, twin))
    first = cp.go(one_send, one_recv, core=twin)
    mine, mine_decay = theirs(*own_state, core), theirs(*own_decay, core)
    first.wait_recv()
    got, got_decay = unpack(r["one"], 1)
    state0, state1 = jnp.where(core == 0, mine, got), jnp.where(core == 0, got, mine)
    decay0, decay1 = jnp.where(core == 0, mine_decay, got_decay), jnp.where(core == 0, got_decay, mine_decay)
    pack(r["two"], yh, decay1 * state0 + state1, decay0 * decay1)
    second = gather_scan(cp, r["two"], yh, nyh, "yh")

    gates = over(nn, reds, lambda c: r["gate_w"][c])
    r["gact"][...] = silu(gates)
    mix = r["mix"]
    for c in range(tokens // 128):
        here = slice(128 * c, 128 * c + 128)
        past = 128 * c + 128
        couple = nt(cact[here], bact[:past])
        seen = lax.broadcasted_iota(jnp.int32, (128, past), 0) + 128 * c >= lax.broadcasted_iota(jnp.int32, (128, past), 1)
        for p in range(2):
            outs = []
            for h in (2 * p, 2 * p + 1):
                spread = cols[here, h : h + 1] - logs[h : h + 1, :past]
                fade = jnp.where(seen, jnp.exp(jnp.minimum(spread, 0.0)), 0.0)
                m = (couple * fade * step[h : h + 1, :past]).astype(BF16)
                outs.append(nn(m, vact[:past, 128 * p : 128 * p + 128]))
            skip = halves(jnp.full((1, 1), r["skip"][2 * p], F32), jnp.full((1, 1), r["skip"][2 * p + 1], F32))
            values = vact[here, 128 * p : 128 * p + 128].astype(F32)
            mix[here, 128 * p : 128 * p + 128] = halves(*outs) + skip * values

    cp.drain()
    for copy in second:
        copy.wait_recv()
    before, before_decay, run, run_decay = prefix(r["two"], yh, nyh)
    pack(r["three"], x, run, run_decay)
    third = gather_scan(cp, r["three"], x, nx, "x")
    for copy in third:
        copy.wait_recv()
    far = prefix(r["three"], x, nx)[0]
    entry0 = before_decay * far + before
    entry1 = decay0 * entry0 + state0
    inc = r["inc"]
    inc[core] = theirs(entry0, entry1, core).astype(BF16)
    r["fin"][...] = theirs(entry0, entry1, twin).astype(BF16)
    fourth = cp.go(r["fin"], inc.at[core], core=twin)
    fourth.wait_recv()

    gated = []
    for p in range(2):
        h = 2 * p
        carried = nn(cact[...], inc[p]) * halves(cols[:, 16 + h : 17 + h], cols[:, 17 + h : 18 + h])
        gated.append((mix[:, 128 * p : 128 * p + 128] + carried) * r["gact"][:, 128 * p : 128 * p + 128])
    gated = jnp.concatenate(gated, axis=1)
    high, low = split2(gated * gated)
    own = token_rows(nt(ones, high) + nt(ones, low))
    r["gq"][0] = jnp.concatenate([own, jnp.zeros_like(own)], axis=0)
    groups = [
        cp.go(r["gq"].at[0], r["gq"].at[1], yl=other),
        cp.go(r["gq"].at[0], r["gq"].at[2], z=mate),
        cp.go(r["gq"].at[0], r["gq"].at[3], z=mate, yl=other),
    ]
    loads["odown"].wait()
    pf = r["pf"]
    pf[...] = nn((gated * r["gain2"][...]).astype(BF16), r["odown"][...])
    nrm = r["nrm"]
    for g in groups_out:
        if g["order"] == "y":
            g["p"][...] = pf[:, g["cols"]].astype(BF16).reshape(g["p"].shape)
    early = [FLOWS["y"](cp, env, g, nrm, None, nothing) for g in groups_out if g["order"] == "y"]
    for flow in early:
        next(flow)
    for copy in groups:
        copy.wait_recv()
    squares = r["gq"][0] + r["gq"][1] + r["gq"][2] + r["gq"][3]
    norm = lax.rsqrt(squares / (width * 4) + EPS)
    norm = jnp.concatenate([norm, jnp.zeros((120, 128), F32)], axis=0).T
    per = 128 // (2 * rows)
    for c in range(tokens // 128):
        by_row = jnp.broadcast_to(norm[:, c : c + 1], (128, 128))
        nrm[per * c : per * c + per] = by_row.reshape(per, 2, rows, 128)
        for g in groups_out:
            if g["order"] == "z":
                scaled = (pf[128 * c : 128 * c + 128, g["cols"]] * by_row[:, :1]).astype(BF16)
                g["p"][per * c : per * c + per] = scaled.reshape(per, *g["p"].shape[1:])
    def finish(g):
        if "oup" not in held:
            held["oup"] = True
            loads["oup"].wait()
            r["out"][...] = nn(g["g"][...].reshape(tokens, -1), r["oup"][g["cols"]])
        else:
            r["out"][...] += nn(g["g"][...].reshape(tokens, -1), r["oup"][g["cols"]])

    late = [FLOWS["z"](cp, env, g, None, None, functools.partial(finish, g)) for g in groups_out if g["order"] == "z"]
    for flow in late + early:
        next(flow)
    run_flows(cp, early + late, ())
    crossing = [g for g in groups_out if g["order"] == "y"]
    oup = r["oup"]
    r["out"][...] += sum(nn(g["g"][...].reshape(tokens, -1), oup[g["cols"]]) for g in crossing)
    cp.drain()


def on_device(sizes, hidden, norm_gain, rank_down, gate_up, value_up, state_up, step_up, conv_value, conv_state, step_bias, decay_log, skip_gain, gate_gain, out_down, out_up):
    nx, nyh, ncore, nz, nyl = sizes
    tokens, width = hidden.shape
    rank = rank_down.shape[1]
    half = state_up.shape[1]
    rows = tokens // (nz * nyl)
    vm, hbm, sm = (pl.BlockSpec(memory_space=s) for s in (pltpu.VMEM, pl.ANY, pltpu.SMEM))
    operands = [
        ("hid_h", hbm, hidden), ("gain", vm, norm_gain.reshape(1, -1)), ("down_h", hbm, rank_down), ("gate_w_h", hbm, gate_up),
        ("value_w_h", hbm, value_up), ("state_w_h", hbm, state_up.T), ("step_w_h", hbm, step_up.T), ("conv_v", vm, conv_value),
        ("conv_s", vm, conv_state), ("bias", sm, step_bias), ("decay", sm, decay_log), ("skip", sm, skip_gain),
        ("gain2", vm, gate_gain.reshape(1, -1)), ("odown_h", hbm, out_down), ("oup_h", hbm, out_up),
    ]
    like = lambda a: pltpu.VMEM(a.shape, a.dtype)
    sends, arrivals = 58, 270
    scratch = [
        ("hid", like(hidden)), ("down", like(rank_down)), ("gate_w", like(gate_up)), ("value_w", like(value_up)), ("state_w", like(state_up.T)),
        ("step_w", like(step_up.T)), ("odown", like(out_down)), ("oup", like(out_up)), *group_buffers("in", nz, rows), *group_buffers("out", nz, rows),
        ("q0", pltpu.VMEM((8, 128), F32)), ("q1", pltpu.VMEM((8, 128), F32)), ("qz", pltpu.VMEM((nz, 8, 128), F32)),
        ("gz", pltpu.VMEM((nz, half, rank // (nx * ncore)), BF16)), ("ss", pltpu.VMEM((nx * ncore, 2, nyl, half, rank // (nx * ncore)), BF16)),
        ("swt", pltpu.VMEM((2 * nyl * half, rank), BF16)), ("fac", pltpu.VMEM((2, rows, 128), F32)),
        ("pre", pltpu.VMEM((16 + tokens, width + 2 * nyl * half), F32)), ("vact", pltpu.VMEM((tokens, width), BF16)),
        ("bact", pltpu.VMEM((tokens, 128), BF16)), ("cact", pltpu.VMEM((tokens, 128), BF16)), ("gact", pltpu.VMEM((tokens, width), F32)),
        ("cols", pltpu.VMEM((tokens, 32), F32)), ("mix", pltpu.VMEM((tokens, width), F32)), ("pf", pltpu.VMEM((tokens, rank), F32)),
        ("nrm", pltpu.VMEM((nz, 2, rows, 128), F32)),
        ("one", pltpu.VMEM((2, 144, 128), BF16)), ("two", pltpu.VMEM((nyh, 144, 128), BF16)), ("three", pltpu.VMEM((nx, 144, 128), BF16)),
        ("fin", pltpu.VMEM((128, 128), BF16)), ("inc", pltpu.VMEM((2, 128, 128), BF16)), ("gq", pltpu.VMEM((4, 8, 128), F32)),
        ("send", pltpu.SemaphoreType.DMA((sends,))), ("recv", pltpu.SemaphoreType.DMA((arrivals,))), ("load_sem", pltpu.SemaphoreType.DMA((8,))),
    ]
    names = [n for n, _, _ in operands] + ["out"] + [n for n, _ in scratch]
    update = pl.pallas_call(
        functools.partial(block_kernel, sizes, names),
        out_shape=jax.ShapeDtypeStruct(hidden.shape, F32),
        in_specs=[s for _, s, _ in operands],
        out_specs=vm,
        scratch_shapes=[s for _, s in scratch],
        compiler_params=pltpu.CompilerParams(collective_id=0, has_side_effects=True, vmem_limit_bytes=60 * 2**20),
    )(*(a for _, _, a in operands))
    return (hidden.astype(F32) + update).astype(BF16)


def grid_sizes(mesh):
    seq, tp = mesh.shape["seq"], mesh.shape["tp"]
    nx = nyh = 1
    if seq == 32:
        nx = nyh = 4
    return (nx, nyh, 2, tp // 2, 2)


def solution(mesh):
    sizes = grid_sizes(mesh)
    finer = Mesh(mesh.devices.reshape(sizes), SEQ + TP)
    rows, cols, flat = P(TP, None), P(None, TP), P(TP)
    placed = (P(SEQ, TP), flat, rows, cols, cols, cols, cols, cols, cols, flat, flat, flat, flat, rows, cols)
    return jax.shard_map(
        functools.partial(on_device, sizes), mesh=finer, in_specs=placed, out_specs=P(SEQ, TP), check_vma=False
    )
```

```python
import functools

import jax
import jax.numpy as jnp
from jax import lax
from jax.experimental import pallas as pl
from jax.experimental.pallas import tpu as pltpu
from jax.sharding import Mesh
from jax.sharding import PartitionSpec as P

GROUPS = 4
EPS = 1e-05
SEQ = ("x", "yh", "core")
TP = ("z", "yl")
F32 = jnp.float32
BF16 = jnp.bfloat16
MESH = pl.DeviceIdType.MESH

ORDER = (3, -3, 4, 2, -2, 1, -1, 0)
SKIP = (True, True)
SKIP_Z = (True, True)
EARLY = 3
PARTS = (("y", 256), ("y", 256), ("y", 256), ("z", 256))


def nt(a, b):
    return lax.dot_general(a, b, (((1,), (1,)), ((), ())), preferred_element_type=F32)


def nn(a, b):
    return jnp.dot(a, b, preferred_element_type=F32)


def silu(x):
    return x * (1.0 / (1.0 + jnp.exp(-x)))


def split2(x):
    high = x.astype(BF16)
    return high, (x - high.astype(F32)).astype(BF16)


class Copies:
    def __init__(self, send, recv):
        self.send, self.recv, self.sent, self.used = send, recv, 0, 0
        self.free, self.all, self.old = [], [], []

    def hold(self, src, dst, **where):
        if self.free:
            self.slot = self.free.pop()
        else:
            self.slot, self.sent = self.sent, self.sent + 1
        self.used += 1
        return pltpu.make_async_remote_copy(
            src_ref=src,
            dst_ref=dst,
            send_sem=self.send.at[self.slot],
            recv_sem=self.recv.at[self.used - 1],
            device_id=where,
            device_id_type=MESH,
        )

    def go(self, src, dst, **where):
        copy = self.hold(src, dst, **where)
        copy.start()
        self.all.append((copy, self.slot))
        return copy

    def turn(self):
        for copy, slot in self.old:
            copy.wait_send()
            self.free.append(slot)
        self.old, self.all = self.all, []

    def drain(self):
        self.turn()
        self.turn()


def up(v):
    return v.astype(F32)


def flow_y_first(cp, env, buf, scale, factor, done):
    z, y, nz = env
    at = lambda off: lax.rem(z + off + nz, nz)
    other = 1 - y
    p, yr, r, h, g = buf["p"], buf["y"], buf["r"], buf["h"], buf["g"]
    part = {1: pl.ds(0, 16), -1: pl.ds(16, 16)}
    across, got = {}, {}
    def cross(first, last):
        for k in range(first, last):
            off = ORDER[k]
            across[off] = (k, cp.go(p.at[at(off), other], yr.at[k], yl=other))

    cross(0, 3)
    yield
    cross(3, EARLY)
    yield

    def own(off):
        k, copy = across[off]
        copy.wait_recv()
        sums = up(p[at(off), y]) + up(yr[k])
        return sums if scale is None else sums * scale[at(off), y][:, :1]

    for d, s in ((0, 1), (1, -1)):
        p[at(3 * s), y] = own(3 * s).astype(BF16)
        got[s, 3] = cp.go(p.at[at(3 * s), y], r.at[d, 0], z=at(s))
    p[at(4), y] = own(4).astype(BF16)
    for s in (1, -1):
        got[s, 4] = cp.go(p.at[at(4), y, part[s]], h.at[part[s]], z=at(2 * s))
    cross(EARLY, len(ORDER))
    yield
    far = 2 if SKIP[0] else 1
    for d, s in ((0, 1), (1, -1)):
        mine = own(2 * s)
        got[s, 3].wait_recv()
        got[s, 4].wait_recv()
        r[d, 0] = (up(r[d, 0]) + mine).astype(BF16)
        r[d, 0, part[s]] = (up(r[d, 0, part[s]]) + up(h[part[s]])).astype(BF16)
        got[s, 2] = cp.go(r.at[d, 0], r.at[d, 1], z=at(far * s))
        if SKIP[0]:
            p[at(s), y] = own(s).astype(BF16)
            got[s, 1] = cp.go(p.at[at(s), y], r.at[d, 2], z=at(s))
    yield
    if not SKIP[0]:
        for d, s in ((0, 1), (1, -1)):
            mine = own(s)
            got[s, 2].wait_recv()
            r[d, 1] = (up(r[d, 1]) + mine).astype(BF16)
            got[s, 1] = cp.go(r.at[d, 1], r.at[d, 2], z=at(s))
        yield
    total = own(0)
    for d, s in ((0, 1), (1, -1)):
        for e in (1, 2) if SKIP[0] else (2,):
            got[s, 3 - e].wait_recv()
            total = total + up(r[d, e])
    if factor is not None:
        total = total * factor()[y]
    mine = g.at[z, y]
    g[z, y] = total.astype(BF16)
    seen = {}
    for hop in (1, 2) if SKIP[1] else (1,):
        for s in (1, -1):
            seen[s, hop] = cp.go(mine, mine, z=at(hop * s))
    last = [cp.go(mine, mine, yl=other)]
    yield
    for k in (1, 2, 3):
        for s in (1, -1):
            seen[s, k].wait_recv()
            block = g.at[at(-k * s), y]
            if k == 1 and not SKIP[1]:
                seen[s, 2] = cp.go(block, block, z=at(s))
            if k == 2:
                half = g.at[at(-2 * s), y, part[s]]
                seen[s, 4] = cp.go(half, half, z=at(2 * s))
                seen[s, 3] = cp.go(block, block, z=at(s))
            last.append(cp.go(block, block, yl=other))
        yield
    for s in (1, -1):
        seen[s, 4].wait_recv()
        half = g.at[at(4), y, part[s]]
        last.append(cp.go(half, half, yl=other))
    yield
    for copy in last:
        copy.wait_recv()
    done()


def flow_z_first(cp, env, buf, scale, factor, done):
    z, y, nz = env
    at = lambda off: lax.rem(z + off + nz, nz)
    p, yr, r, h, g = buf["p"], buf["y"], buf["r"], buf["h"], buf["g"]
    part = {1: pl.ds(0, 16), -1: pl.ds(16, 16)}
    every = slice(None)
    got, seen = {}, {}
    for d, s in ((0, 1), (1, -1)):
        got[s, 4] = cp.go(p.at[at(4), :, part[s]], h.at[:, part[s]], z=at(2 * s))
        got[s, 3] = cp.go(p.at[at(3 * s)], r.at[d, 0], z=at(s))
    if SKIP_Z[0]:
        for d, s in ((0, 1), (1, -1)):
            got[s, 1] = cp.go(p.at[at(s)], r.at[d, 2], z=at(s))
    yield
    far = 2 if SKIP_Z[0] else 1
    for d, s in ((0, 1), (1, -1)):
        got[s, 3].wait_recv()
        got[s, 4].wait_recv()
        r[d, 0] = (up(r[d, 0]) + up(p[at(2 * s)])).astype(BF16)
        r[d, 0, :, part[s]] = (up(r[d, 0, :, part[s]]) + up(h[:, part[s]])).astype(BF16)
        got[s, 2] = cp.go(r.at[d, 0], r.at[d, 1], z=at(far * s))
    yield
    if not SKIP_Z[0]:
        for d, s in ((0, 1), (1, -1)):
            got[s, 2].wait_recv()
            r[d, 1] = (up(r[d, 1]) + up(p[at(s)])).astype(BF16)
            got[s, 1] = cp.go(r.at[d, 1], r.at[d, 2], z=at(s))
        yield
    total = up(p[z])
    for d, s in ((0, 1), (1, -1)):
        for e in (1, 2) if SKIP_Z[0] else (2,):
            got[s, 3 - e].wait_recv()
            total = total + up(r[d, e])
    yr[0] = total.astype(BF16)
    swap = cp.go(yr.at[0], yr.at[1], yl=1 - y)
    yield
    swap.wait_recv()
    total = up(yr[0]) + up(yr[1])
    if factor is not None:
        total = total * factor()[...]
    g[z] = total.astype(BF16)
    for hop in (1, 2) if SKIP_Z[1] else (1,):
        for s in (1, -1):
            seen[s, hop] = cp.go(g.at[z], g.at[z], z=at(hop * s))
    yield
    for k in (1, 2, 3):
        for s in (1, -1):
            seen[s, k].wait_recv()
            block = g.at[at(-k * s)]
            if k == 1 and not SKIP_Z[1]:
                seen[s, 2] = cp.go(block, block, z=at(s))
            if k == 2:
                half = g.at[at(-2 * s), :, part[s]]
                seen[s, 4] = cp.go(half, half, z=at(2 * s))
                seen[s, 3] = cp.go(block, block, z=at(s))
        yield
    for s in (1, -1):
        seen[s, 4].wait_recv()
    done()


def run_flows(cp, flows, hooks):
    turn = 0
    while flows:
        cp.turn()
        hooks[turn]() if turn < len(hooks) else None
        turn += 1
        left = []
        for flow in flows:
            if next(flow, flow) is not flow:
                left.append(flow)
        flows = left


def gather_scan(cp, buf, place, peers, axis):
    copies = []
    for o in sorted(range(1, peers), key=lambda o: -min(o, peers - o)):
        there = lax.rem(place + o, peers)
        copies.append(cp.go(buf.at[place], buf.at[place], **{axis: there}))
    return copies


def pack(ref, where, state, decay):
    high, low = split2(decay)
    ref[where, pl.ds(0, 128), :] = state.astype(BF16)
    row = lax.broadcasted_iota(jnp.int32, (16, 128), 0)
    tail = jnp.where(row == 0, high.astype(F32), jnp.where(row == 1, low.astype(F32), 0.0))
    ref[where, pl.ds(128, 16), :] = tail.astype(BF16)


def unpack(ref, where):
    tail = ref[where, pl.ds(128, 16), :].astype(F32)
    return ref[where, pl.ds(0, 128), :].astype(F32), tail[0:1] + tail[1:2]


def prefix(buf, place, peers):
    run, decay = jnp.zeros((128, 128), F32), jnp.ones((1, 128), F32)
    before, before_decay = run, decay
    for k in range(peers):
        here = place == k
        before = jnp.where(here, run, before)
        before_decay = jnp.where(here, decay, before_decay)
        state, d = unpack(buf, k)
        run, decay = d * run + state, d * decay
    return before, before_decay, run, decay


FLOWS = {"y": flow_y_first, "z": flow_z_first}


class Column:
    def __init__(self, ref):
        self.ref = ref

    def __getitem__(self, k):
        return self.ref[k][..., :1]


def group_buffers(side, nz, rows):
    out = []
    for i, (order, c) in enumerate(PARTS):
        both = (2, rows, c) if order == "z" else (rows, c)
        shapes = dict(p=(nz, 2, rows, c), g=(nz, 2, rows, c), r=(2, 3, *both), h=both, y=(2, *both) if order == "z" else (nz, *both))
        if side == "in":
            shapes["halo"] = (16, c)
        out += [(f"{side}{i}{k}", pltpu.VMEM(v, BF16)) for k, v in shapes.items()]
    return out


def split_groups(r, side):
    out, start = [], 0
    for i, (order, c) in enumerate(PARTS):
        g = {k: r[f"{side}{i}{k}"] for k in ("p", "g", "r", "h", "y", "halo") if f"{side}{i}{k}" in r}
        out.append(dict(g, order=order, cols=slice(start, start + c)))
        start += c
    return out


def seq_shift(sizes, place, by):
    nx, nyh, ncore = sizes[:3]
    total = nx * nyh * ncore
    there = lax.rem(place + by + total, total)
    return dict(x=there // (nyh * ncore), yh=lax.rem(there // ncore, nyh), core=lax.rem(there, ncore))


def token_rows(v):
    return jnp.concatenate([v[0:1, 128 * c : 128 * c + 128] for c in range(v.shape[1] // 128)], axis=0)


def halves(low, high):
    lane = lax.broadcasted_iota(jnp.int32, (low.shape[0], 128), 1)
    return jnp.where(lane < 64, low, high)


def block_kernel(sizes, names, *args):
    r = dict(zip(names, args))
    nx, nyh, ncore, nz, nyl = sizes
    x, yh, core, z, y = (lax.axis_index(a) for a in ("x", "yh", "core", "z", "yl"))
    other, twin = 1 - y, 1 - core
    hid, groups_in, groups_out = r["hid"], split_groups(r, "in"), split_groups(r, "out")
    tokens, width = hid.shape
    rows, rank = groups_in[0]["p"].shape[2], r["down"].shape[1]
    env = (z, y, nz)
    place = (x * nyh + yh) * ncore + core
    at = lambda off: lax.rem(z + off + nz, nz)
    mate = z + 1 - 2 * lax.rem(z, 2)
    cp = Copies(r["send"], r["recv"])

    shares = [(o, c) for o in range(nx) for c in range(ncore) if o or c]
    share_peer = lambda o, c: dict(x=lax.rem(x + o, nx), core=lax.rem(core + c, ncore))
    peers = [dict(z=at(o)) for o in range(1, nz)] + [dict(yl=other), dict(z=mate, yl=other)]
    peers += [dict(yh=lax.rem(yh + o, nyh)) for o in range(1, nyh)]
    peers += [share_peer(o, c) for o, c in shares]
    peers += [seq_shift(sizes, place, 1), seq_shift(sizes, place, -1)]
    barrier = pltpu.get_barrier_semaphore()
    for peer in peers:
        pl.semaphore_signal(barrier, inc=1, device_id=peer, device_id_type=MESH)

    loads = {}
    for k, name in enumerate(("hid", "down", "state_w", "value_w", "step_w", "gate_w", "odown", "oup")):
        loads[name] = pltpu.make_async_copy(r[name + "_h"], r[name], r["load_sem"].at[k])
        if k < 2:
            loads[name].start()

    loads["hid"].wait()
    loads["down"].wait()
    for name in ("state_w", "value_w", "step_w", "gate_w", "odown", "oup"):
        loads[name].start()
    wide = hid[...].astype(F32)
    ones = jnp.ones((8, width), BF16)
    high, low = split2(wide * wide)
    squares = token_rows(nt(ones, high) + nt(ones, low))
    taps = r["conv_s"][...]
    blank = jnp.zeros_like(taps)
    taps = jnp.where(y == 0, jnp.concatenate([taps, blank], axis=1), jnp.concatenate([blank, taps], axis=1))
    r["q0"][...] = jnp.concatenate([squares, taps], axis=0)
    part = nn((wide * r["gain"][...]).astype(BF16), r["down"][...]).astype(BF16)
    for g in groups_in:
        g["p"][...] = part[:, g["cols"]].reshape(g["p"].shape)
    share = x * ncore + core
    half = r["state_w"].shape[0]
    span = rank // (nx * ncore)
    loads["state_w"].wait()
    gz = r["gz"]
    gz[z] = r["state_w"][:, pl.ds(pl.multiple_of(share * span, span), span)]
    pl.semaphore_wait(barrier, len(peers))

    picked = z // 2
    held = {}
    nothing = lambda: None

    def hook0():
        held["q"] = cp.go(r["q0"], r["q1"], yl=other)
        held["gz"] = []
        for o in range(1, nz):
            copy = cp.hold(gz.at[z], gz.at[z], z=at(o))
            sends = at(o) // 2 == lax.rem(z, 4)
            comes = lax.rem(at(-o), 4) == picked
            held["gz"].append((sends, comes, copy))

            @pl.when(sends)
            def _():
                copy.start()

    def hook1():
        held["q"].wait_recv()
        r["qz"][z] = r["q0"][...] + r["q1"][...]
        held["qz"] = [cp.go(r["qz"].at[z], r["qz"].at[z], z=at(o)) for o in range(1, nz)]

    def hook2():
        for sends, comes, copy in held["gz"]:
            @pl.when(comes)
            def _():
                copy.wait_recv()

            @pl.when(sends)
            def _():
                copy.wait_send()

        for k in range(2):
            r["ss"][share, k, y] = gz[4 * k + picked]
        held["ss"] = cp.go(r["ss"].at[share, :, y], r["ss"].at[share, :, y], yl=other)

    def hook3():
        held["ss"].wait_recv()
        held["shares"] = [cp.go(r["ss"].at[share], r["ss"].at[share], **share_peer(o, c)) for o, c in shares]

    fac = r["fac"]

    def factor():
        if "factor" not in held:
            held["factor"] = True
            for copy in held["qz"]:
                copy.wait_recv()
            summed = r["qz"][0]
            for k in range(1, nz):
                summed = summed + r["qz"][k]
            near = 2 * rows
            per = 128 // near
            row = jnp.zeros((1, 128), F32)
            for c in range(tokens // 128):
                row = jnp.where(z // per == c, summed[c : c + 1], row)
            wanted = lax.broadcasted_iota(jnp.int32, (near, 128), 1) == lax.broadcasted_iota(jnp.int32, (near, 128), 0) + near * lax.rem(z, per)
            mean = jnp.sum(jnp.where(wanted, row, 0.0), axis=1, keepdims=True) / (width * nz * nyl)
            fac[...] = jnp.broadcast_to(lax.rsqrt(mean + EPS), (near, 128)).reshape(2, rows, 128)
        return Column(fac)

    value_w = r["value_w"]
    pre = r["pre"]
    gact = r["gact"]

    def begin(g):
        block = g["g"][...].reshape(tokens, -1)
        if "begun" not in held:
            held["begun"] = True
            for name in ("value_w", "step_w", "gate_w"):
                loads[name].wait()
            pre[16:, :width] = nn(block, value_w[g["cols"]])
        else:
            pre[16:, :width] += nn(block, value_w[g["cols"]])

    flows = {o: [FLOWS[o](cp, env, g, None, factor, functools.partial(begin, g) if o == "z" else nothing) for g in groups_in if g["order"] == o] for o in "zy"}
    for flow in flows["z"] + flows["y"] + flows["y"]:
        next(flow)
    run_flows(cp, flows["y"] + flows["z"], (hook0, hook1, hook2, hook3))

    last = pl.ds(rows - 16, 16)
    following = seq_shift(sizes, place, 1)
    halos = [cp.go(g["g"].at[nz - 1, 1, last], g["halo"], **following) for g in groups_in]
    reds = [g["g"][...].reshape(tokens, -1) for g in groups_in]
    cuts = [g["cols"] for g in groups_in]
    over = lambda f, blocks, take: sum(f(b, take(c)) for b, c in zip(blocks, cuts))

    for copy in held["shares"]:
        copy.wait_recv()
    swt = r["swt"]
    for k in range(nx * ncore):
        swt[:, span * k : span * (k + 1)] = r["ss"][k].reshape(2 * nyl * half, span)
    pre = r["pre"]
    chans = 2 * nyl * half
    value_w = r["value_w"]

    def project(blocks):
        return over(nn, blocks, lambda c: value_w[c]), over(nt, blocks, lambda c: swt[:, c])

    pre[16:, :width] += sum(nn(b, value_w[g["cols"]]) for b, g in zip(reds, groups_in) if g["order"] == "y")
    pre[16:, width:] = over(nt, reds, lambda c: swt[:, c])

    heads = r["step_w"].shape[0]
    step_t = jnp.concatenate([r["step_w"][...].astype(F32), jnp.zeros((8 - heads, rank), F32)], axis=0).astype(BF16)
    raw = over(lambda b, w: nt(w, b), reds, lambda c: step_t[:, c])
    head = lax.broadcasted_iota(jnp.int32, (8, 1), 0)
    bias, decay = jnp.zeros((8, 1), F32), jnp.zeros((8, 1), F32)
    for h in range(heads):
        bias = jnp.where(head == h, r["bias"][h], bias)
        decay = jnp.where(head == h, r["decay"][h], decay)
    raw = raw + bias
    step = jnp.maximum(raw, 0.0) + jnp.log1p(jnp.exp(-jnp.abs(raw)))
    lane = lax.broadcasted_iota(jnp.int32, (8, tokens), 1)
    logs = -jnp.exp(decay) * step
    k = 1
    while k < tokens:
        logs = logs + jnp.where(lane >= k, pltpu.roll(logs, k, axis=1), 0.0)
        k *= 2
    final = logs[:, tokens - 1 : tokens]
    ending = jnp.exp(final - logs) * step
    stack = jnp.concatenate([logs, ending, jnp.exp(logs), jnp.zeros((8, tokens), F32)], axis=0)
    cols = r["cols"]
    cols[...] = stack.T
    whole = jnp.exp(final)

    vact, bact, cact = r["vact"], r["bact"], r["cact"]
    weights = r["conv_v"][...]
    sweights = jnp.concatenate([r["qz"][picked][4:8], r["qz"][4 + picked][4:8]], axis=1)

    def convolve(c):
        acc_v = jnp.zeros((128, width), F32)
        acc_s = jnp.zeros((128, chans), F32)
        for t in range(4):
            window = pre[13 + t + 128 * c : 13 + t + 128 * c + 128, :]
            acc_v = acc_v + weights[t : t + 1] * window[:, :width]
            acc_s = acc_s + sweights[t : t + 1] * window[:, width:]
        here = slice(128 * c, 128 * c + 128)
        vact[here] = silu(acc_v).astype(BF16)
        acts = silu(acc_s).astype(BF16)
        bact[here] = acts[:, :128]
        cact[here] = acts[:, 128:]

    for c in range(1, tokens // 128):
        convolve(c)
    for copy in halos:
        copy.wait_recv()
    hv, hs = project([g["halo"][...] for g in groups_in])
    keep = jnp.where(place == 0, 0.0, 1.0)
    pre[:16, :width] = hv * keep
    pre[:16, width:] = hs * keep
    convolve(0)

    eye = (lax.broadcasted_iota(jnp.int32, (128, 128), 0) == lax.broadcasted_iota(jnp.int32, (128, 128), 1)).astype(BF16)
    b_t = nt(eye, bact[...]).astype(BF16)
    own_state, own_decay = [], []
    for p in range(2):
        h = 2 * p
        ends = halves(cols[:, 8 + h : 9 + h], cols[:, 9 + h : 10 + h])
        scaled = (vact[:, 128 * p : 128 * p + 128].astype(F32) * ends).astype(BF16)
        own_state.append(nn(b_t, scaled))
        own_decay.append(halves(whole[h : h + 1], whole[h + 1 : h + 2]))
    theirs = lambda a, b, c: jnp.where(c == 0, a, b)
    one_send, one_recv = r["one"].at[0], r["one"].at[1]
    pack(r["one"], 0, theirs(*own_state, twin), theirs(*own_decay, twin))
    first = cp.go(one_send, one_recv, core=twin)
    mine, mine_decay = theirs(*own_state, core), theirs(*own_decay, core)
    first.wait_recv()
    got, got_decay = unpack(r["one"], 1)
    state0, state1 = jnp.where(core == 0, mine, got), jnp.where(core == 0, got, mine)
    decay0, decay1 = jnp.where(core == 0, mine_decay, got_decay), jnp.where(core == 0, got_decay, mine_decay)
    pack(r["two"], yh, decay1 * state0 + state1, decay0 * decay1)
    second = gather_scan(cp, r["two"], yh, nyh, "yh")

    gates = over(nn, reds, lambda c: r["gate_w"][c])
    r["gact"][...] = silu(gates)
    mix = r["mix"]
    for c in range(tokens // 128):
        here = slice(128 * c, 128 * c + 128)
        past = 128 * c + 128
        couple = nt(cact[here], bact[:past])
        seen = lax.broadcasted_iota(jnp.int32, (128, past), 0) + 128 * c >= lax.broadcasted_iota(jnp.int32, (128, past), 1)
        for p in range(2):
            outs = []
            for h in (2 * p, 2 * p + 1):
                spread = cols[here, h : h + 1] - logs[h : h + 1, :past]
                fade = jnp.where(seen, jnp.exp(jnp.minimum(spread, 0.0)), 0.0)
                m = (couple * fade * step[h : h + 1, :past]).astype(BF16)
                outs.append(nn(m, vact[:past, 128 * p : 128 * p + 128]))
            skip = halves(jnp.full((1, 1), r["skip"][2 * p], F32), jnp.full((1, 1), r["skip"][2 * p + 1], F32))
            values = vact[here, 128 * p : 128 * p + 128].astype(F32)
            mix[here, 128 * p : 128 * p + 128] = halves(*outs) + skip * values

    cp.drain()
    for copy in second:
        copy.wait_recv()
    before, before_decay, run, run_decay = prefix(r["two"], yh, nyh)
    pack(r["three"], x, run, run_decay)
    third = gather_scan(cp, r["three"], x, nx, "x")
    for copy in third:
        copy.wait_recv()
    far = prefix(r["three"], x, nx)[0]
    entry0 = before_decay * far + before
    entry1 = decay0 * entry0 + state0
    inc = r["inc"]
    inc[core] = theirs(entry0, entry1, core).astype(BF16)
    r["fin"][...] = theirs(entry0, entry1, twin).astype(BF16)
    fourth = cp.go(r["fin"], inc.at[core], core=twin)
    fourth.wait_recv()

    gated = []
    for p in range(2):
        h = 2 * p
        carried = nn(cact[...], inc[p]) * halves(cols[:, 16 + h : 17 + h], cols[:, 17 + h : 18 + h])
        gated.append((mix[:, 128 * p : 128 * p + 128] + carried) * r["gact"][:, 128 * p : 128 * p + 128])
    gated = jnp.concatenate(gated, axis=1)
    high, low = split2(gated * gated)
    own = token_rows(nt(ones, high) + nt(ones, low))
    r["gq"][0] = jnp.concatenate([own, jnp.zeros_like(own)], axis=0)
    groups = [
        cp.go(r["gq"].at[0], r["gq"].at[1], yl=other),
        cp.go(r["gq"].at[0], r["gq"].at[2], z=mate),
        cp.go(r["gq"].at[0], r["gq"].at[3], z=mate, yl=other),
    ]
    loads["odown"].wait()
    pf = r["pf"]
    pf[...] = nn((gated * r["gain2"][...]).astype(BF16), r["odown"][...])
    nrm = r["nrm"]
    for g in groups_out:
        if g["order"] == "y":
            g["p"][...] = pf[:, g["cols"]].astype(BF16).reshape(g["p"].shape)
    early = [FLOWS["y"](cp, env, g, nrm, None, nothing) for g in groups_out if g["order"] == "y"]
    for flow in early:
        next(flow)
    for copy in groups:
        copy.wait_recv()
    squares = r["gq"][0] + r["gq"][1] + r["gq"][2] + r["gq"][3]
    norm = lax.rsqrt(squares / (width * 4) + EPS)
    norm = jnp.concatenate([norm, jnp.zeros((120, 128), F32)], axis=0).T
    per = 128 // (2 * rows)
    for c in range(tokens // 128):
        by_row = jnp.broadcast_to(norm[:, c : c + 1], (128, 128))
        nrm[per * c : per * c + per] = by_row.reshape(per, 2, rows, 128)
        for g in groups_out:
            if g["order"] == "z":
                scaled = (pf[128 * c : 128 * c + 128, g["cols"]] * by_row[:, :1]).astype(BF16)
                g["p"][per * c : per * c + per] = scaled.reshape(per, *g["p"].shape[1:])
    def finish(g):
        if "oup" not in held:
            held["oup"] = True
            loads["oup"].wait()
            r["pf"][:, :width] = nn(g["g"][...].reshape(tokens, -1), r["oup"][g["cols"]])
        else:
            r["pf"][:, :width] += nn(g["g"][...].reshape(tokens, -1), r["oup"][g["cols"]])

    late = [FLOWS["z"](cp, env, g, None, None, functools.partial(finish, g)) for g in groups_out if g["order"] == "z"]
    for flow in late + early:
        next(flow)
    run_flows(cp, early + late, ())
    crossing = [g for g in groups_out if g["order"] == "y"]
    oup = r["oup"]
    update = pf[:, :width] + sum(nn(g["g"][...].reshape(tokens, -1), oup[g["cols"]]) for g in crossing)
    r["out"][...] = update.astype(BF16)
    cp.drain()


def on_device(sizes, hidden, norm_gain, rank_down, gate_up, value_up, state_up, step_up, conv_value, conv_state, step_bias, decay_log, skip_gain, gate_gain, out_down, out_up):
    nx, nyh, ncore, nz, nyl = sizes
    tokens, width = hidden.shape
    rank = rank_down.shape[1]
    half = state_up.shape[1]
    rows = tokens // (nz * nyl)
    vm, hbm, sm = (pl.BlockSpec(memory_space=s) for s in (pltpu.VMEM, pl.ANY, pltpu.SMEM))
    operands = [
        ("hid_h", hbm, hidden), ("gain", vm, norm_gain.reshape(1, -1)), ("down_h", hbm, rank_down), ("gate_w_h", hbm, gate_up),
        ("value_w_h", hbm, value_up), ("state_w_h", hbm, state_up.T), ("step_w_h", hbm, step_up.T), ("conv_v", vm, conv_value),
        ("conv_s", vm, conv_state), ("bias", sm, step_bias), ("decay", sm, decay_log), ("skip", sm, skip_gain),
        ("gain2", vm, gate_gain.reshape(1, -1)), ("odown_h", hbm, out_down), ("oup_h", hbm, out_up),
    ]
    like = lambda a: pltpu.VMEM(a.shape, a.dtype)
    sends, arrivals = 58, 270
    scratch = [
        ("hid", like(hidden)), ("down", like(rank_down)), ("gate_w", like(gate_up)), ("value_w", like(value_up)), ("state_w", like(state_up.T)),
        ("step_w", like(step_up.T)), ("odown", like(out_down)), ("oup", like(out_up)), *group_buffers("in", nz, rows), *group_buffers("out", nz, rows),
        ("q0", pltpu.VMEM((8, 128), F32)), ("q1", pltpu.VMEM((8, 128), F32)), ("qz", pltpu.VMEM((nz, 8, 128), F32)),
        ("gz", pltpu.VMEM((nz, half, rank // (nx * ncore)), BF16)), ("ss", pltpu.VMEM((nx * ncore, 2, nyl, half, rank // (nx * ncore)), BF16)),
        ("swt", pltpu.VMEM((2 * nyl * half, rank), BF16)), ("fac", pltpu.VMEM((2, rows, 128), F32)),
        ("pre", pltpu.VMEM((16 + tokens, width + 2 * nyl * half), F32)), ("vact", pltpu.VMEM((tokens, width), BF16)),
        ("bact", pltpu.VMEM((tokens, 128), BF16)), ("cact", pltpu.VMEM((tokens, 128), BF16)), ("gact", pltpu.VMEM((tokens, width), F32)),
        ("cols", pltpu.VMEM((tokens, 32), F32)), ("mix", pltpu.VMEM((tokens, width), F32)), ("pf", pltpu.VMEM((tokens, rank), F32)),
        ("nrm", pltpu.VMEM((nz, 2, rows, 128), F32)),
        ("one", pltpu.VMEM((2, 144, 128), BF16)), ("two", pltpu.VMEM((nyh, 144, 128), BF16)), ("three", pltpu.VMEM((nx, 144, 128), BF16)),
        ("fin", pltpu.VMEM((128, 128), BF16)), ("inc", pltpu.VMEM((2, 128, 128), BF16)), ("gq", pltpu.VMEM((4, 8, 128), F32)),
        ("send", pltpu.SemaphoreType.DMA((sends,))), ("recv", pltpu.SemaphoreType.DMA((arrivals,))), ("load_sem", pltpu.SemaphoreType.DMA((8,))),
    ]
    names = [n for n, _, _ in operands] + ["out"] + [n for n, _ in scratch]
    update = pl.pallas_call(
        functools.partial(block_kernel, sizes, names),
        out_shape=jax.ShapeDtypeStruct(hidden.shape, BF16),
        in_specs=[s for _, s, _ in operands],
        out_specs=vm,
        scratch_shapes=[s for _, s in scratch],
        compiler_params=pltpu.CompilerParams(collective_id=0, has_side_effects=True, vmem_limit_bytes=60 * 2**20),
    )(*(a for _, _, a in operands))
    return (hidden.astype(F32) + update.astype(F32)).astype(BF16)


def grid_sizes(mesh):
    seq, tp = mesh.shape["seq"], mesh.shape["tp"]
    nx = nyh = 1
    if seq == 32:
        nx = nyh = 4
    return (nx, nyh, 2, tp // 2, 2)


def solution(mesh):
    sizes = grid_sizes(mesh)
    finer = Mesh(mesh.devices.reshape(sizes), SEQ + TP)
    rows, cols, flat = P(TP, None), P(None, TP), P(TP)
    placed = (P(SEQ, TP), flat, rows, cols, cols, cols, cols, cols, cols, flat, flat, flat, flat, rows, cols)
    return jax.shard_map(
        functools.partial(on_device, sizes), mesh=finer, in_specs=placed, out_specs=P(SEQ, TP), check_vma=False
    )
```
